32 devices in a mesh: rep: 4 (over x, y), dp: 8 (over z, core).
Axes of the slice: x: 2, y: 2, z: 4, core: 2. Of those that a mesh axis runs over, the one named last changes fastest.
Arguments:
- x: bfloat16 [32, 2048, 640], P(('rep', 'dp')), parts along dimension 0
- dy: bfloat16 [32, 2048, 640], P(('rep', 'dp')), parts along dimension 0
- w_gate: bfloat16 [2, 640, 2560], replicated
- w_up: bfloat16 [2, 640, 2560], replicated
- w_down: bfloat16 [2, 2560, 640], replicated
- m_w_gate: float32 [2, 640, 2560], P(None, 'dp')
- m_w_up: float32 [2, 640, 2560], P(None, 'dp')
- m_w_down: float32 [2, 2560, 640], P(None, 'dp')
- v_w_gate: float32 [2, 640, 2560], P(None, 'dp')
- v_w_up: float32 [2, 640, 2560], P(None, 'dp')
- v_w_down: float32 [2, 2560, 640], P(None, 'dp')
Outputs:
- output 1: bfloat16 [8, 640, 2560], P('rep'), parts along dimension 0
- output 2: bfloat16 [8, 640, 2560], P('rep'), parts along dimension 0
- output 3: bfloat16 [8, 2560, 640], P('rep'), parts along dimension 0
- output 4: float32 [8, 640, 2560], P('rep', 'dp'), parts along dimension 0
- output 5: float32 [8, 640, 2560], P('rep', 'dp'), parts along dimension 0
- output 6: float32 [8, 2560, 640], P('rep', 'dp'), parts along dimension 0
- output 7: float32 [8, 640, 2560], P('rep', 'dp'), parts along dimension 0
- output 8: float32 [8, 640, 2560], P('rep', 'dp'), parts along dimension 0
- output 9: float32 [8, 2560, 640], P('rep', 'dp'), parts along dimension 0
There are 4 independent parts. The reference program is written for one: setup_inputs(seed, part) draws one part's arguments, and reference() takes and returns one part's arrays. A program takes and returns all parts, laid end to end along the dimension named above; an argument that names none is the same for every part.
All inputs are finite; a program needn't handle non-finite values.
Results may differ from the reference program's by a relative error of at most 0.022.
Values are sent between devices in bfloat16 or wider.
A program may use at most 2 GiB of HBM per device.

```python
import jax
import jax.numpy as jnp
from jax import lax

SEQUENCES = 8
TOKENS = 2048
D = 640
FF = 2560
LAYERS = 2
NAMES = ("w_gate", "w_up", "w_down")
SHAPES = {"w_gate": (LAYERS, D, FF), "w_up": (LAYERS, D, FF), "w_down": (LAYERS, FF, D)}


def bump(key, n, height):
    away = (jnp.arange(n, dtype=jnp.int32) - jax.random.randint(key, (), 0, n, jnp.int32)) % n
    return jnp.where(away < n // 8, height, 1.0)


def together(key, own, strength):
    shared = jax.random.normal(key, own.shape[1:], jnp.float32)
    return (own + strength * shared) * lax.rsqrt(1 + strength * strength)


def setup_inputs(seed: int = 0, part: int = 0) -> dict:
    kx, kdy, ka, kb, kz, kf, kh, kl, *keys = jax.random.split(jax.random.key(seed), 8 + 3 * len(NAMES))
    kx, kdy, ka, kb = (jax.random.fold_in(k, part) for k in (kx, kdy, ka, kb))
    kw, km, kv = (keys[i::3] for i in range(3))
    shape = (SEQUENCES, TOKENS, D)
    much_x, much_dy = jax.random.uniform(kz, (2,), jnp.float32, 0.0, 1.0)
    loud = 2.0 ** jax.random.uniform(jax.random.fold_in(kz, 1), (), jnp.float32, -1.0, 2.0)
    layers = 2.0 ** jax.random.uniform(kl, (LAYERS, 1, 1), jnp.float32, -1.0, 1.0)
    x = together(ka, jax.random.normal(kx, shape, jnp.float32), much_x) * bump(kf, D, 4.0)
    dy = together(kb, jax.random.normal(kdy, shape, jnp.float32), much_dy)
    drawn = {"x": x.astype(jnp.bfloat16), "dy": (loud * dy * (SEQUENCES * TOKENS) ** -0.5).astype(jnp.bfloat16)}
    for key, name in zip(kw, NAMES, strict=True):
        w = jax.random.normal(key, SHAPES[name], jnp.float32) * SHAPES[name][1] ** -0.5
        drawn[name] = (w * {"w_gate": 1.0, "w_up": bump(kh, FF, 4.0), "w_down": layers}[name]).astype(jnp.bfloat16)
    for key, name in zip(km, NAMES, strict=True):
        drawn[f"m_{name}"] = 0.1 * jax.random.normal(key, SHAPES[name], jnp.float32)
    for key, name in zip(kv, NAMES, strict=True):
        drawn[f"v_{name}"] = jax.random.uniform(key, SHAPES[name], jnp.float32, 0.005, 0.015)
    return drawn


def matmul(a, w):
    return jnp.dot(a, w, preferred_element_type=jnp.float32).astype(jnp.bfloat16)


def normed(h):
    wide = h.astype(jnp.float32)
    scale = lax.rsqrt(jnp.mean(wide**2, -1, keepdims=True) + 1e-6)
    return (wide * scale).astype(jnp.bfloat16)


def layer(h, w):
    a = normed(h)
    gate = jnp.dot(a, w["w_gate"], preferred_element_type=jnp.float32)
    up = jnp.dot(a, w["w_up"], preferred_element_type=jnp.float32)
    return h + matmul((jax.nn.silu(gate) * up).astype(jnp.bfloat16), w["w_down"])


def adamw(w, m, v, g):
    m = 0.9 * m + 0.1 * g
    v = 0.95 * v + 0.05 * g * g
    step = m * lax.rsqrt(v + 1e-8) + 0.1 * w
    return (w - 0.02 * step).astype(jnp.bfloat16), m, v


def clipped(gradients, sum_of_squares, count):
    factor = jnp.minimum(1.0, 0.5 * lax.rsqrt(sum_of_squares / count + 1e-30))
    return [g * factor for g in gradients]


def stack(weights, h):
    return lax.scan(lambda h, w: (layer(h, w), None), h, weights)[0]


def reference(x, dy, w_gate, w_up, w_down, m_w_gate, m_w_up, m_w_down, v_w_gate, v_w_up, v_w_down):
    weights = dict(zip(NAMES, (w_gate, w_up, w_down), strict=True))

    def take(so_far, sequence):
        h, by_y = sequence
        _, back = jax.vjp(lambda w: stack(w, h), weights)
        return jax.tree.map(lambda total, term: total + term.astype(jnp.float32), so_far, back(by_y)[0]), None

    none_yet = {name: jnp.zeros(w.shape, jnp.float32) for name, w in weights.items()}
    by_weights, _ = lax.scan(take, none_yet, (x, dy))
    gradients = [by_weights[name].astype(jnp.bfloat16).astype(jnp.float32) for name in NAMES]
    gradients = clipped(gradients, sum(jnp.sum(g * g) for g in gradients), sum(g.size for g in gradients))
    new = [
        adamw(w.astype(jnp.float32), m, v, g)
        for w, m, v, g in zip((w_gate, w_up, w_down), (m_w_gate, m_w_up, m_w_down), (v_w_gate, v_w_up, v_w_down), gradients, strict=True)
    ]
    return tuple(one[which] for which in range(3) for one in new)
```

```python
import functools

import jax
import jax.numpy as jnp
from jax import lax
from jax.experimental import pallas as pl
from jax.experimental.pallas import tpu as pltpu
from jax.sharding import PartitionSpec as P

f32, bf16 = jnp.float32, jnp.bfloat16
D, F, Q = 640, 2560, 640
LAYERS = 2
ITEMS = 8
SLOTS = 5
TM = 512
COLS = ((0, 256), (256, 256), (512, 128))


def dot(a, b):
    return jnp.dot(a, b, preferred_element_type=f32)


def dot_bt(a, b):
    return lax.dot_general(a, b, (((1,), (1,)), ((), ())), preferred_element_type=f32)


def dot_at(a, b):
    return lax.dot_general(a, b, (((0,), (0,)), ((), ())), preferred_element_type=f32)


def rows(t, n):
    return pl.ds(pl.multiple_of(t * n, n), n)


def loop(n, body):
    lax.fori_loop(0, n, lambda i, _: (body(i), 0)[1], 0)


def place():
    me = lax.axis_index("dp")
    return me, lax.div(me, 2), lax.rem(me, 2)


def quarter(i):
    r = lax.rem(i, 4)
    odd, half = lax.rem(r, 2), lax.div(r, 2)
    return (1 - odd) * (2 + half) + odd * (1 - half)


def step_kernel(
    x, dy, wg, wu, wd, og, ou, od, oss,
    h_v, a_v, dy_v, big, da_v, wgu_v, wdb_v, wda_v, own, ownd, pair, paird, got, gotd, ss_v,
    in_sem, w_sem, psend, precv, ssend, srecv, fsem, credit, pcredit,
):
    tokens = x.shape[0]
    me, z, c = place()
    partner = {"dp": me + 1 - 2 * c}

    def weights(l, q, slot, down=True):
        cols = rows(q, Q)
        two = (
            pltpu.make_async_copy(wg.at[l, :, cols], wgu_v.at[slot, :, 0:Q], w_sem.at[slot, 0]),
            pltpu.make_async_copy(wu.at[l, :, cols], wgu_v.at[slot, :, Q : 2 * Q], w_sem.at[slot, 1]),
        )
        return two + (pltpu.make_async_copy(wd.at[l, cols], wdb_v.at[slot], w_sem.at[slot, 2]),) if down else two

    load_x = pltpu.make_async_copy(x, h_v, in_sem.at[0])
    load_dy = pltpu.make_async_copy(dy, dy_v, in_sem.at[1])
    load_wd = pltpu.make_async_copy(wd.at[0], wda_v, in_sem.at[2])
    load_x.start()
    for copy in weights(0, 0, 0, False):
        copy.start()
    load_wd.start()
    load_dy.start()

    ss_v[...] = jnp.zeros_like(ss_v)
    got[...] = jnp.zeros_like(got)
    gotd[...] = jnp.zeros_like(gotd)
    barrier = pltpu.get_barrier_semaphore()
    pl.semaphore_signal(barrier, inc=1, device_id=partner)

    @pl.when(z > 0)
    def _():
        pl.semaphore_signal(barrier, inc=1, device_id={"dp": me - 2})

    @pl.when(z < 3)
    def _():
        pl.semaphore_signal(barrier, inc=1, device_id={"dp": me + 2})

    def zero(t):
        da_v[rows(t, 128)] = jnp.zeros((128, D), f32)

    loop(tokens // 128, zero)
    load_x.wait()

    def norm(l):
        def tile(t):
            r = rows(t, 256)
            wide = h_v[r].astype(f32)
            a_v[l, r] = (wide * lax.rsqrt(jnp.mean(wide * wide, -1, keepdims=True) + 1e-6)).astype(bf16)

        loop(tokens // 256, tile)

    norm(0)

    def forward(n):
        slot = lax.rem(n, 2)
        for copy in weights(0, n, slot, False):
            copy.wait()

        @pl.when(n < 3)
        def _():
            for copy in weights(0, n + 1, 1 - slot, False):
                copy.start()

        def tile(t):
            r = rows(t, TM)
            a = a_v[0, r]
            for c0, cn in COLS:
                g = dot(a, wgu_v[slot, :, c0 : c0 + cn])
                u = dot(a, wgu_v[slot, :, Q + c0 : Q + c0 + cn])
                big[r, pl.ds(pl.multiple_of(n * Q + c0, 128), cn)] = (g / (1 + jnp.exp(-g)) * u).astype(bf16)

        loop(tokens // TM, tile)

    loop(4, forward)
    for copy in weights(1, quarter(0), 0):
        copy.start()
    load_wd.wait()

    def down(t):
        r = rows(t, TM)
        h_v[r] = h_v[r] + dot(big[r], wda_v[...]).astype(bf16)

    loop(tokens // TM, down)
    norm(1)
    load_dy.wait()
    near = 2 + lax.convert_element_type((z > 0) & (z < 3), jnp.int32)
    pl.semaphore_wait(barrier, near)

    def item_of(s, way):
        return (1 - way) * (s - 1 - z) + way * (s - 4 + z)

    def is_last(way):
        return z == 3 * (1 - way)

    def is_first(way):
        return z == 3 * way

    def has_d(i, way):
        return lax.rem(i, 2) == way

    def send_gu(way, i, b):
        slot, r = lax.rem(i, SLOTS), lax.rem(i, 2)
        return pltpu.make_async_remote_copy(
            own.at[slot, 2 * (1 - way) + b, c], got.at[way, r, b], ssend.at[way, slot, b], srecv.at[way, r, b],
            device_id={"dp": me + 2 - 4 * way},
        )

    def send_d(way, i):
        slot, r = lax.rem(i, SLOTS), lax.rem(i, 2)
        return pltpu.make_async_remote_copy(
            ownd.at[slot, c], gotd.at[r], ssend.at[way, slot, 2], srecv.at[way, r, 2],
            device_id={"dp": me + 2 - 4 * way},
        )

    def keep_gu(way, i, b):
        slot, q = lax.rem(i, SLOTS), quarter(i)
        j, l = way * b + (1 - way) * (1 - b), 1 - lax.div(i, 4)
        src = own.at[slot, 2 * (1 - way) + b, c]
        return (
            pltpu.make_async_copy(src.at[:, 0:Q], og.at[j, l, :, rows(q, Q)], fsem.at[slot, 2 * b]),
            pltpu.make_async_copy(src.at[:, Q : 2 * Q], ou.at[j, l, :, rows(q, Q)], fsem.at[slot, 2 * b + 1]),
        )

    def keep_d(way, i):
        slot, q = lax.rem(i, SLOTS), quarter(i)
        j, l = way * q + (1 - way) * (3 - q), 1 - lax.div(i, 4)
        return pltpu.make_async_copy(ownd.at[slot, c], od.at[j, l], fsem.at[slot, 4])

    def swap(i):
        slot = lax.rem(i, SLOTS)
        return (
            pltpu.make_async_remote_copy(own.at[slot, :, 1 - c], pair.at[slot], psend.at[slot, 0], precv.at[slot, 0], device_id=partner),
            pltpu.make_async_remote_copy(ownd.at[slot, 1 - c], paird.at[slot], psend.at[slot, 1], precv.at[slot, 1], device_id=partner),
        )

    def settle(i):
        for copy in swap(i):
            copy.wait_send()

        def one(way):
            @pl.when(is_last(way))
            def _():
                for b in range(2):
                    for copy in keep_gu(way, i, b):
                        copy.wait()

                @pl.when(has_d(i, way))
                def _():
                    keep_d(way, i).wait()

            @pl.when(jnp.logical_not(is_last(way)))
            def _():
                for b in range(2):
                    send_gu(way, i, b).wait_send()

                @pl.when(has_d(i, way))
                def _():
                    send_d(way, i).wait_send()

        loop(2, one)

    def stage(way, i):
        slot, r = lax.rem(i, SLOTS), lax.rem(i, 2)

        @pl.when(jnp.logical_not(is_last(way)) & (i >= 2))
        def _():
            pl.semaphore_wait(credit.at[way], 1)

        def gu(b):
            @pl.when(jnp.logical_not(is_first(way)))
            def _():
                send_gu(way, i, b).wait_recv()

            zb = 2 * (1 - way) + b

            def part(k):
                at = rows(k, 16)
                total = own[slot, zb, c, at].astype(f32) + pair[slot, zb, at].astype(f32) + got[way, r, b, at].astype(f32)
                total = total.astype(bf16)
                own[slot, zb, c, at] = total

                @pl.when(is_last(way))
                def _():
                    g = total.astype(f32)
                    ss_v[...] += jnp.sum((g * g).reshape(2, 8, 2 * Q), 0)

            loop(5, part)

            @pl.when(is_last(way))
            def _():
                for copy in keep_gu(way, i, b):
                    copy.start()

            @pl.when(jnp.logical_not(is_last(way)))
            def _():
                send_gu(way, i, b).start()

        loop(2, gu)

        @pl.when(has_d(i, way))
        def _():
            @pl.when(jnp.logical_not(is_first(way)))
            def _():
                send_d(way, i).wait_recv()

            def part(k):
                at = rows(k, 32)
                other = jnp.where(is_first(way), 0.0, gotd[r, at].astype(f32))
                total = (ownd[slot, c, at].astype(f32) + paird[slot, at].astype(f32) + other).astype(bf16)
                ownd[slot, c, at] = total

                @pl.when(is_last(way))
                def _():
                    g = total.astype(f32)
                    ss_v[:, 0:D] += jnp.sum((g * g).reshape(4, 8, D), 0)

            loop(10, part)

            @pl.when(is_last(way))
            def _():
                keep_d(way, i).start()

            @pl.when(jnp.logical_not(is_last(way)))
            def _():
                send_d(way, i).start()

        @pl.when(jnp.logical_not(is_first(way)) & (i < ITEMS - 2))
        def _():
            pl.semaphore_signal(credit.at[way], inc=1, device_id={"dp": me - 2 + 4 * way})

    def engine(s):
        @pl.when((s >= 1) & (s <= ITEMS))
        def _():
            for copy in swap(s - 1):
                copy.wait_recv()

        def one(way):
            i = item_of(s, way)

            @pl.when((i >= 0) & (i < ITEMS))
            def _():
                stage(way, i)

        loop(2, one)

        @pl.when((s >= SLOTS - 1) & (s < ITEMS - 1))
        def _():
            pl.semaphore_signal(pcredit, inc=1, device_id=partner)

    def backward_norm():
        def tile(t):
            r = rows(t, 256)
            wide, da = h_v[r].astype(f32), da_v[r].astype(bf16).astype(f32)
            scale = lax.rsqrt(jnp.mean(wide * wide, -1, keepdims=True) + 1e-6)
            dot_mean = jnp.mean(da * wide, -1, keepdims=True)
            dwide = scale * da - wide * (scale * scale * scale * dot_mean)
            dy_v[r] = (dy_v[r].astype(f32) + dwide.astype(bf16).astype(f32)).astype(bf16)

        loop(tokens // 256, tile)

    def step(s):
        l, slot, at = 1 - lax.div(s, 4), lax.rem(s, SLOTS), lax.rem(s, 2)

        @pl.when(s < ITEMS)
        def _():
            for copy in weights(l, quarter(s), at):
                copy.wait()

            @pl.when(s < ITEMS - 1)
            def _():
                for copy in weights(1 - lax.div(s + 1, 4), quarter(s + 1), 1 - at):
                    copy.start()

            @pl.when(s == 4)
            def _():
                backward_norm()

            def tile(t):
                r = rows(t, TM)
                a, dh = a_v[l, r], dy_v[r]
                for c0, cn in COLS:
                    g = dot(a, wgu_v[at, :, c0 : c0 + cn])
                    u = dot(a, wgu_v[at, :, Q + c0 : Q + c0 + cn])
                    d = dot_bt(dh, wdb_v[at, c0 : c0 + cn]).astype(bf16).astype(f32)
                    sig = 1 / (1 + jnp.exp(-g))
                    silu = g * sig
                    big[r, 2 * Q + c0 : 2 * Q + c0 + cn] = (silu * u).astype(bf16)
                    big[r, Q + c0 : Q + c0 + cn] = (d * silu).astype(bf16)
                    big[r, c0 : c0 + cn] = (d * u * (sig + silu * (1 - sig))).astype(bf16)

            loop(tokens // TM, tile)

        engine(s)

        @pl.when(s < ITEMS)
        def _():
            @pl.when(s >= SLOTS)
            def _():
                settle(s - SLOTS)
                pl.semaphore_wait(pcredit, 1)

            for n in range(5):
                k = 128 * n
                value = dot_at(big[:, 2 * Q + k : 2 * Q + k + 128], dy_v[...]).astype(bf16)
                for half in range(2):
                    lo, hi = max(k, 320 * half), min(k + 128, 320 * half + 320)
                    if lo < hi:
                        ownd[slot, half, lo - 320 * half : hi - 320 * half] = value[lo - k : hi - k]

            def cols(n):
                k = pl.ds(pl.multiple_of(n * 256, 256), 256)
                own[slot, :, :, :, k] = dot_at(a_v[l], big[:, k]).astype(bf16).reshape(4, 2, 80, 256)

            loop(5, cols)
            for copy in swap(s):
                copy.start()

            @pl.when(s < 4)
            def _():
                def tile(t):
                    r = rows(t, TM)
                    da_v[r] += dot_bt(big[r, 0 : 2 * Q], wgu_v[at])

                loop(tokens // TM, tile)

    loop(ITEMS + 4, step)
    loop(SLOTS, lambda k: settle(ITEMS - SLOTS + k))
    oss[...] = ss_v[...]


def reduce_gradients(x, dy, wg, wu, wd):
    tokens = x.shape[0]
    hbm, vmem, dma = pl.BlockSpec(memory_space=pl.ANY), pl.BlockSpec(memory_space=pltpu.VMEM), pltpu.SemaphoreType.DMA
    return pl.pallas_call(
        step_kernel,
        name="step_kernel",
        out_shape=(
            jax.ShapeDtypeStruct((2, LAYERS, 80, F), bf16),
            jax.ShapeDtypeStruct((2, LAYERS, 80, F), bf16),
            jax.ShapeDtypeStruct((2, LAYERS, 320, D), bf16),
            jax.ShapeDtypeStruct((8, 2 * Q), f32),
        ),
        in_specs=[hbm] * 5,
        out_specs=(hbm, hbm, hbm, vmem),
        scratch_shapes=[
            pltpu.VMEM((tokens, D), bf16),
            pltpu.VMEM((2, tokens, D), bf16),
            pltpu.VMEM((tokens, D), bf16),
            pltpu.VMEM((tokens, F), bf16),
            pltpu.VMEM((tokens, D), f32),
            pltpu.VMEM((2, D, 2 * Q), bf16),
            pltpu.VMEM((2, Q, D), bf16),
            pltpu.VMEM((F, D), bf16),
            pltpu.VMEM((SLOTS, 4, 2, 80, 2 * Q), bf16),
            pltpu.VMEM((SLOTS, 2, 320, D), bf16),
            pltpu.VMEM((SLOTS, 4, 80, 2 * Q), bf16),
            pltpu.VMEM((SLOTS, 320, D), bf16),
            pltpu.VMEM((2, 2, 2, 80, 2 * Q), bf16),
            pltpu.VMEM((2, 320, D), bf16),
            pltpu.VMEM((8, 2 * Q), f32),
            dma((3,)),
            dma((2, 3)),
            dma((SLOTS, 2)),
            dma((SLOTS, 2)),
            dma((2, SLOTS, 3)),
            dma((2, 2, 3)),
            dma((SLOTS, 5)),
            pltpu.SemaphoreType.REGULAR((2,)),
            pltpu.SemaphoreType.REGULAR,
        ],
        compiler_params=pltpu.CompilerParams(collective_id=0, has_side_effects=True, vmem_limit_bytes=67043328),
    )(x, dy, wg, wu, wd)


def gather_kernel(
    ss, eg, eu, ed, wg, wu, wd, mg, mu, md, vg, vu, vd, og, ou, od, qg, qu, qd, oc,
    gg, gu, gd, bg, bu, bd, fg, fu, fd, sg, su, sd, sums, part,
    sum_send, sum_recv, g_sem, g_send, in_sem, z_send, z_recv, p_send, p_recv, q_sem,
):
    me, z, c = place()
    partner = {"dp": me + 1 - 2 * c}
    end = (z == 0) | (z == 3)
    inner = me + 2 - 4 * lax.div(z, 3)
    ends, gs, outs = (eg, eu, ed), (gg, gu, gd), (og, ou, od)

    def cut(ref, mat, half, lead, first):
        if mat < 2:
            return ref.at[(*lead, pl.ds(pl.multiple_of(first * 80, 16), 80), rows(half, 1280))]
        return ref.at[(*lead, pl.ds(pl.multiple_of(first * 320 + half * 160, 32), 160), slice(None))]

    def state(mat):
        n = 80 if mat < 2 else 320
        w = (wg, wu, wd)[mat].at[:, pl.ds(pl.multiple_of(me * n, 16), n)]
        return (
            pltpu.make_async_copy((mg, mu, md)[mat], (fg, fu, fd)[mat], in_sem.at[mat, 0]),
            pltpu.make_async_copy((vg, vu, vd)[mat], (sg, su, sd)[mat], in_sem.at[mat, 1]),
            pltpu.make_async_copy(w, (bg, bu, bd)[mat], in_sem.at[mat, 2]),
        )

    def own_g(mat):
        return pltpu.make_async_copy(ends[mat].at[0], gs[mat], q_sem.at[mat, 0])

    def keep_g(mat):
        return pltpu.make_async_copy(gs[mat], (qg, qu, qd)[mat], q_sem.at[mat, 1])

    def hand_g(k, mat):
        l, half = lax.div(k, 2), lax.rem(k, 2)
        return pltpu.make_async_remote_copy(
            cut(ends[mat], mat, half, (1, l), 0), cut(gs[mat], mat, half, (l,), 0), g_send.at[k, mat], g_sem.at[k, mat],
            device_id={"dp": inner},
        )

    def send_sum(k):
        return pltpu.make_async_remote_copy(
            part, sums.at[me], sum_send.at[k], sum_recv.at[me], device_id={"dp": lax.rem(me + k, 8)}
        )

    def get_sum(k):
        of = lax.rem(me + k, 8)
        return pltpu.make_async_remote_copy(part, sums.at[of], sum_send.at[k], sum_recv.at[of], device_id={"dp": of})

    def chunk(k, mat, block):
        l, half = lax.div(k, 2), lax.rem(k, 2)
        return cut(outs[mat], mat, half, (l,), block)

    def along(way, hop, k, mat, block):
        ref = chunk(k, mat, block)
        return pltpu.make_async_remote_copy(
            ref, ref, z_send.at[way, hop, k, mat], z_recv.at[way, hop, k, mat], device_id={"dp": me + 2 - 4 * way}
        )

    def across(k, mat, block):
        ref = chunk(k, mat, block)
        of = lax.div(block, 2)
        return pltpu.make_async_remote_copy(ref, ref, p_send.at[of, k, mat], p_recv.at[of, k, mat], device_id=partner)

    part[...] = sum(ss[:, 128 * n : 128 * n + 128] for n in range(2 * Q // 128))
    for mat in range(3):
        for copy in state(mat):
            copy.start()
    barrier = pltpu.get_barrier_semaphore()
    for k in range(1, 8):
        pl.semaphore_signal(barrier, inc=1, device_id={"dp": lax.rem(me + k, 8)})
    pl.semaphore_wait(barrier, 7)
    for k in range(1, 8):
        send_sum(k).start()

    @pl.when(end)
    def _():
        for mat in range(3):
            own_g(mat).start()

        def hand(k):
            for mat in range(3):
                hand_g(k, mat).start()

        loop(4, hand)

    sums[me] = part[...]
    for k in range(1, 8):
        get_sum(k).wait_recv()
    total = jnp.zeros((1, 1), f32)
    for k in range(8):
        total += jnp.sum(jnp.sum(sums[k], 0, keepdims=True), 1, keepdims=True)
    count = LAYERS * 3 * D * F
    factor = jnp.minimum(1.0, 0.5 * lax.rsqrt(total * (1.0 / count) + 1e-30))
    oc[...] = jnp.broadcast_to(factor, oc.shape)
    for mat in range(3):
        for copy in state(mat):
            copy.wait()

    @pl.when(end)
    def _():
        for mat in range(3):
            own_g(mat).wait()

    def adamw(k):
        l, half = lax.div(k, 2), lax.rem(k, 2)
        for mat in range(3):
            @pl.when(jnp.logical_not(end))
            def _():
                hand_g(k, mat).wait_recv()

            def piece(n):
                if mat < 2:
                    r, col = rows(n, 16), rows(half, 1280)
                    to = (l, pl.ds(pl.multiple_of(me * 80 + n * 16, 16), 16), col)
                else:
                    r, col = pl.ds(pl.multiple_of(half * 160 + n * 32, 32), 32), slice(None)
                    to = (l, pl.ds(pl.multiple_of(me * 320 + half * 160 + n * 32, 32), 32), col)
                g = gs[mat][l, r, col].astype(f32) * oc[0:1, 0:1]
                w = (bg, bu, bd)[mat][l, r, col].astype(f32)
                m = 0.9 * (fg, fu, fd)[mat][l, r, col] + 0.1 * g
                v = 0.95 * (sg, su, sd)[mat][l, r, col] + 0.05 * g * g
                outs[mat][to] = (w - 0.02 * (m * lax.rsqrt(v + 1e-8) + 0.1 * w)).astype(bf16)

            loop(5, piece)

            @pl.when(z > 0)
            def _():
                along(1, 0, k, mat, me).start()

            @pl.when(z < 3)
            def _():
                along(0, 0, k, mat, me).start()

            across(k, mat, me).start()

    loop(4, adamw)
    for mat in range(3):
        keep_g(mat).start()

    def onward(n):
        hop, k = lax.div(n, 4) + 1, lax.rem(n, 4)
        for mat in range(3):
            @pl.when(z + hop <= 3)
            def _():
                block = me + 2 * hop
                along(1, hop - 1, k, mat, block).wait_recv()

                @pl.when(z > 0)
                def _():
                    along(1, hop, k, mat, block).start()

                across(k, mat, block).start()

            @pl.when(z - hop >= 0)
            def _():
                block = me - 2 * hop
                along(0, hop - 1, k, mat, block).wait_recv()

                @pl.when(z < 3)
                def _():
                    along(0, hop, k, mat, block).start()

                across(k, mat, block).start()

    loop(12, onward)

    def finish(n):
        of, k = lax.div(n, 4), lax.rem(n, 4)
        for mat in range(3):
            across(k, mat, 2 * of + c).wait_send()
            across(k, mat, 2 * of + 1 - c).wait_recv()

            @pl.when((of >= z) & (z > 0))
            def _():
                along(1, of - z, k, mat, 2 * of + c).wait_send()

            @pl.when((of <= z) & (z < 3))
            def _():
                along(0, z - of, k, mat, 2 * of + c).wait_send()

    loop(16, finish)
    for k in range(1, 8):
        send_sum(k).wait_send()
    for mat in range(3):
        keep_g(mat).wait()

    @pl.when(end)
    def _():
        def hand(k):
            for mat in range(3):
                hand_g(k, mat).wait_send()

        loop(4, hand)


def gather_weights(ss, g, w, m, v):
    hbm, vmem, dma = pl.BlockSpec(memory_space=pl.ANY), pl.BlockSpec(memory_space=pltpu.VMEM), pltpu.SemaphoreType.DMA
    block = [(LAYERS, 80, F), (LAYERS, 80, F), (LAYERS, 320, D)]
    return pl.pallas_call(
        gather_kernel,
        name="gather_kernel",
        out_shape=(
            pltpu.VMEM((LAYERS, D, F), bf16),
            pltpu.VMEM((LAYERS, D, F), bf16),
            pltpu.VMEM((LAYERS, F, D), bf16),
            *(jax.ShapeDtypeStruct(s, bf16) for s in block),
            jax.ShapeDtypeStruct((8, 128), f32),
        ),
        in_specs=[vmem] + [hbm] * 12,
        out_specs=(vmem, vmem, vmem, hbm, hbm, hbm, vmem),
        scratch_shapes=[
            *(pltpu.VMEM(s, bf16) for s in block),
            *(pltpu.VMEM(s, bf16) for s in block),
            *(pltpu.VMEM(s, f32) for s in block),
            *(pltpu.VMEM(s, f32) for s in block),
            pltpu.VMEM((8, 8, 128), f32),
            pltpu.VMEM((8, 128), f32),
            dma((8,)),
            dma((8,)),
            dma((4, 3)),
            dma((4, 3)),
            dma((3, 3)),
            dma((2, 4, 4, 3)),
            dma((2, 4, 4, 3)),
            dma((4, 4, 3)),
            dma((4, 4, 3)),
            dma((3, 2)),
        ],
        compiler_params=pltpu.CompilerParams(collective_id=1, has_side_effects=True, vmem_limit_bytes=36 << 20),
    )(ss, *g, *w, *m, *v)


def solution(mesh):
    def body(x, dy, *arrays):
        w, m, v = arrays[0:3], arrays[3:6], arrays[6:9]
        *ends, ss = reduce_gradients(x[0], dy[0], *w)
        *rest, factor = gather_weights(ss, ends, w, m, v)
        new_w, own = rest[0:3], rest[3:6]
        c = factor[0, 0]
        g = [t.astype(f32) * c for t in own]
        new_m = [0.9 * a + 0.1 * b for a, b in zip(m, g, strict=True)]
        new_v = [0.95 * a + 0.05 * b * b for a, b in zip(v, g, strict=True)]
        return (*new_w, *new_m, *new_v)

    rep, part = P("rep", None, None), P("rep", "dp", None)
    whole, block = P(None, None, None), P(None, "dp", None)
    seq = P(("rep", "dp"), None, None)
    return jax.shard_map(
        body,
        mesh=mesh,
        in_specs=(seq, seq, *[whole] * 3, *[block] * 6),
        out_specs=(*[rep] * 3, *[part] * 6),
        check_vma=False,
    )
```

```python
import functools

import jax
import jax.numpy as jnp
from jax import lax
from jax.experimental import pallas as pl
from jax.experimental.pallas import tpu as pltpu
from jax.sharding import PartitionSpec as P

f32, bf16 = jnp.float32, jnp.bfloat16
D, F, Q = 640, 2560, 640
LAYERS = 2
R, DROWS, DHALF = 80, 320, 160
WIDE, EVEN, EDGE = 1280, 512, 768
LANES, TILE, PACK, EIGHT = 128, 256, 16, 8
KINDS, BOTH = range(3), range(2)
HEAD = 4
LAG = 6
ITEMS = 8
SLOTS = 4
TM = 1024
COLS = ((0, TILE), (TILE, TILE), (EVEN, LANES))


def dot(a, b):
    return jnp.dot(a, b, preferred_element_type=f32)


def dot_bt(a, b):
    return lax.dot_general(a, b, (((1,), (1,)), ((), ())), preferred_element_type=f32)


def dot_at(a, b):
    return lax.dot_general(a, b, (((0,), (0,)), ((), ())), preferred_element_type=f32)


def sigmoid(g):
    return 0.5 * jnp.tanh(0.5 * g) + 0.5


def odd(i):
    return lax.rem(i, 2)


def half(i):
    return lax.div(i, 2)


def span(start, n):
    return pl.ds(pl.multiple_of(start, LANES if n % LANES == 0 else PACK), n)


def rows(t, n):
    return pl.ds(pl.multiple_of(t * n, n), n)


def loop(n, body):
    lax.fori_loop(0, n, lambda i, _: (body(i), 0)[1], 0)


def place():
    me = lax.axis_index("dp")
    return me, half(me), odd(me)


def quarter(i):
    r = lax.rem(i, 4)
    o, h = odd(r), half(r)
    return (1 - o) * (2 + h) + o * (1 - h)


def step_kernel(
    x, dy, wg, wu, wd, og, ou, od, oss, gate_h, up_h, act_h,
    h_v, a_v, dy_v, big, stage, wgu_v, wdb_v, wda_v, own, pair, got, ss_v,
    in_sem, w_sem, save_sem, psend, precv, send_sem, recv_sem, keep_sem, hsend, hrecv, credit, dcredit, pcredit,
):
    tokens = x.shape[0]
    tiles = tokens // TM
    me, z, c = place()
    partner = {"dp": me + 1 - 2 * c}

    def weights(l, q, slot, down=True):
        cols = rows(q, Q)
        first = pl.ds(pl.multiple_of(q * Q, LANES), EVEN)
        last = pl.ds(pl.multiple_of(q * Q + EVEN, LANES), LANES)
        two = (
            pltpu.make_async_copy(wg.at[l, :, cols], wgu_v.at[slot, :, 0:D], w_sem.at[slot, 0]),
            pltpu.make_async_copy(wu.at[l, :, last], wgu_v.at[slot, :, D:EDGE], w_sem.at[slot, 1]),
            pltpu.make_async_copy(wu.at[l, :, first], wgu_v.at[slot, :, EDGE:WIDE], w_sem.at[slot, 2]),
        )
        return two + (pltpu.make_async_copy(wd.at[l, cols], wdb_v.at[slot], w_sem.at[slot, 3]),) if down else two

    da_v = stage.at[0]

    def held(n, t):
        b, at = odd(t), rows(t, TM)
        return [(stage.at[b, k * TM : k * TM + TM], ref.at[n, at], save_sem.at[b, k]) for k, ref in ((0, gate_h), (1, up_h))]

    def save(n, t):
        return [pltpu.make_async_copy(here, there, sem) for here, there, sem in held(n, t)]

    def fetch(n, t):
        return [pltpu.make_async_copy(there, here, sem) for here, there, sem in held(n, t)]

    def save_act(n):
        return pltpu.make_async_copy(big.at[:, rows(n, Q)], act_h.at[n], save_sem.at[2, 0])

    def fetch_act(n):
        return pltpu.make_async_copy(act_h.at[n], big.at[:, 2 * Q : 3 * Q], save_sem.at[2, 1])

    load_x = pltpu.make_async_copy(x, h_v, in_sem.at[0])
    load_dy = pltpu.make_async_copy(dy, dy_v, in_sem.at[1])
    load_wd = pltpu.make_async_copy(wd.at[0], wda_v, in_sem.at[2])
    load_x.start()
    for copy in weights(0, 0, 0, False):
        copy.start()
    load_wd.start()
    load_dy.start()

    ss_v[...] = jnp.zeros_like(ss_v)

    def clear(k):
        for way in BOTH:
            got[way, k] = jnp.zeros((R, D), bf16)

    loop(PACK, clear)
    barrier = pltpu.get_barrier_semaphore()
    pl.semaphore_signal(barrier, device_id=partner)

    @pl.when(z > 0)
    def _():
        pl.semaphore_signal(barrier, device_id={"dp": me - 2})

    @pl.when(z < 3)
    def _():
        pl.semaphore_signal(barrier, device_id={"dp": me + 2})

    load_x.wait()

    def norm(l):
        def tile(t):
            r = rows(t, TILE)
            wide = h_v[r].astype(f32)
            a = (wide * lax.rsqrt(jnp.mean(wide * wide, -1, keepdims=True) + 1e-6)).astype(bf16)
            a_v[l, r] = a

        loop(tokens // TILE, tile)

    norm(0)

    def gate_up(a, slot):
        for c0, cn in COLS:
            if cn == TILE:
                yield c0, cn, dot(a, wgu_v[slot, :, c0 : c0 + TILE]), dot(a, wgu_v[slot, :, EDGE + c0 : 1024 + c0])
            else:
                both = dot(a, wgu_v[slot, :, EVEN:EDGE])
                yield c0, cn, both[:, 0:LANES], both[:, LANES:TILE]

    def forward(n):
        slot = odd(n)
        for copy in weights(0, n, slot, False):
            copy.wait()

        @pl.when(n < 3)
        def _():
            for copy in weights(0, n + 1, 1 - slot, False):
                copy.start()

        def tile(t):
            @pl.when((n > 0) | (t >= 2))
            def _():
                for copy in save(n, t):
                    copy.wait()

            r = rows(t, TM)
            b = odd(t)
            a = a_v[0, r]
            for c0, cn, g, u in gate_up(a, slot):
                big[r, pl.ds(pl.multiple_of(n * Q + c0, LANES), cn)] = (g * sigmoid(g) * u).astype(bf16)
                stage[b, 0:TM, c0 : c0 + cn] = g
                stage[b, TM : 2 * TM, c0 : c0 + cn] = u
            for copy in save(n, t):
                copy.start()

        loop(tiles, tile)

        @pl.when(n > 0)
        def _():
            save_act(n - 1).wait()

        save_act(n).start()

    loop(4, forward)
    for copy in weights(1, quarter(0), 0):
        copy.start()
    load_wd.wait()

    def down(t):
        r = rows(t, TM)
        h_v[r] = h_v[r] + dot(big[r], wda_v[...]).astype(bf16)

    loop(tiles, down)
    norm(1)
    for t in (tiles - 2, tiles - 1):
        for copy in save(3, t):
            copy.wait()
    save_act(3).wait()

    def zero(t):
        da_v[rows(t, LANES)] = jnp.zeros((LANES, D), f32)

    loop(tokens // LANES, zero)
    load_dy.wait()
    near = 2 + lax.convert_element_type((z > 0) & (z < 3), jnp.int32)
    pl.semaphore_wait(barrier, near)

    def is_last(way):
        return z == 3 * (1 - way)

    def is_first(way):
        return z == 3 * way

    def onward(way):
        return {"dp": me + 2 - 4 * way}

    def half_of(ref, k, h):
        return ref.at[(*k, slice(None), pl.ds(pl.multiple_of(D * h, LANES), D))]

    def send(way, item, k, h, u, g):
        slot = lax.rem(item, SLOTS)
        return pltpu.make_async_remote_copy(
            half_of(own, (slot, k, c), h), got.at[way, g], send_sem.at[way, slot, u], recv_sem.at[way, g], device_id=onward(way)
        )

    def keep(way, item, k, u, kind):
        slot, q, l = lax.rem(item, SLOTS), quarter(item), 1 - lax.div(item, 4)
        if kind == 0:
            j, p = way * q + (1 - way) * (3 - q), u - 4
            out = od.at[j, l, pl.ds(pl.multiple_of(p * R, PACK), R)]
            return [pltpu.make_async_copy(half_of(own, (slot, k, c), odd(p)), out, keep_sem.at[slot, u])]
        b = odd(u)
        j = way * b + (1 - way) * (1 - b)
        mine, out = own.at[slot, k, c], (og, ou)[kind - 1].at[j, l]
        if kind == 1:
            return [pltpu.make_async_copy(mine.at[:, 0:D], out.at[:, rows(q, Q)], keep_sem.at[slot, u])]
        first = pl.ds(pl.multiple_of(q * Q, LANES), EVEN)
        last = pl.ds(pl.multiple_of(q * Q + EVEN, LANES), LANES)
        return [
            pltpu.make_async_copy(mine.at[:, EDGE:WIDE], out.at[:, first], keep_sem.at[slot, u]),
            pltpu.make_async_copy(mine.at[:, D:EDGE], out.at[:, last], keep_sem.at[slot, 6 + u]),
        ]

    def gu_unit(way, item, u):
        return 2 * (1 - way) + odd(u), half(u), odd(item) * 4 + u

    def d_unit(item, p):
        return 4 + half(p), odd(p), EIGHT + odd(half(item)) * 4 + p

    def swap(item, kind):
        slot = lax.rem(item, SLOTS)
        if kind == 0:
            src, dst = own.at[slot, 4:6, 1 - c], pair.at[slot, 4:6]
        else:
            cols = slice(D * (kind - 1), D * kind)
            src, dst = own.at[slot, 0:4, 1 - c, :, cols], pair.at[slot, 0:4, :, cols]
        return pltpu.make_async_remote_copy(src, dst, psend.at[slot, kind], precv.at[slot, kind], device_id=partner)

    def settle(item):
        for kind in KINDS:
            swap(item, kind).wait_send()

        def one(way):
            @pl.when(is_last(way))
            def _():
                for u in range(4):
                    for copy in keep(way, item, gu_unit(way, item, u)[0], u, 1 + u // 2):
                        copy.wait()

                @pl.when(odd(item) == way)
                def _():
                    for p in range(4):
                        for copy in keep(way, item, d_unit(item, p)[0], 4 + p, 0):
                            copy.wait()

            @pl.when(jnp.logical_not(is_last(way)))
            def _():
                for u in range(4):
                    k, h, g = gu_unit(way, item, u)
                    send(way, item, k, h, u, g).wait_send()

                @pl.when(odd(item) == way)
                def _():
                    for p in range(4):
                        k, h, g = d_unit(item, p)
                        send(way, item, k, h, 4 + p, g).wait_send()

        loop(2, one)

    def unit(way, n):
        i, j = lax.div(n, 6), lax.rem(n, 6)
        late = odd(i + way)
        first, last = is_first(way), is_last(way)
        passes = jnp.logical_not(last)
        back = {"dp": me - 2 + 4 * way}

        @pl.when(passes & (i >= 2) & (j == 2))
        def _():
            pl.semaphore_wait(credit.at[way])

        @pl.when(passes & (i >= 4) & (j == 0) & (late == 0))
        def _():
            pl.semaphore_wait(dcredit.at[way])

        is_d = lax.convert_element_type(j < 2, jnp.int32)
        item = i - is_d * late
        some = lax.convert_element_type(item >= 0, jnp.int32)
        more = is_d * (1 - late) * lax.div(i, ITEMS - 1)
        v = lax.max(j - 2, 0)

        def one(x, _):
            p = 2 * late + j + 2 * x
            k, h, g = (is_d * a + (1 - is_d) * b for a, b in zip(d_unit(item, p), gu_unit(way, item, v), strict=True))
            u = is_d * (4 + p) + (1 - is_d) * v
            slot = lax.rem(item, SLOTS)
            mine, other = half_of(own, (slot, k, c), h), half_of(pair, (slot, k), h)

            @pl.when(jnp.logical_not(first))
            def _():
                send(way, item, k, h, u, g).wait_recv()

            total = (mine[...].astype(f32) + other[...].astype(f32) + got[way, g].astype(f32)).astype(bf16)
            mine[...] = total

            @pl.when(passes)
            def _():
                send(way, item, k, h, u, g).start()

            @pl.when(last)
            def _():
                wide = mine[...].astype(f32)
                ss_v[...] += jnp.sum((wide * wide).reshape(10, EIGHT, D), 0)
                for kind in KINDS:
                    @pl.when(half(j) == kind)
                    def _():
                        for copy in keep(way, item, k, u, kind):
                            copy.start()

            return 0

        lax.fori_loop(0, some * (1 + more), one, 0)

        @pl.when(jnp.logical_not(first) & (i < ITEMS - 2) & (j == 5))
        def _():
            pl.semaphore_signal(credit.at[way], device_id=back)

        @pl.when(jnp.logical_not(first) & (late == 1) & (i >= 1) & (i <= 4) & (j == 1))
        def _():
            pl.semaphore_signal(dcredit.at[way], device_id=back)

    upper = half(z)

    def engine(e):
        n = e - HEAD
        for kind in KINDS:
            @pl.when((n >= 0) & (n < 6 * ITEMS) & (lax.rem(n, 6) == 2 * kind))
            def _():
                swap(lax.div(n, 6), kind).wait_recv()

        def one(j):
            way = upper * j + (1 - upper) * (1 - j)
            hops = way * (3 - z) + (1 - way) * z
            mine = n - half(LAG * hops)

            @pl.when((mine >= 0) & (mine < 6 * ITEMS))
            def _():
                unit(way, mine)

        loop(2, one)

    def backward_norm():
        def tile(t):
            r = rows(t, TILE)
            wide, da = h_v[r].astype(f32), da_v[r].astype(bf16).astype(f32)
            scale = lax.rsqrt(jnp.mean(wide * wide, -1, keepdims=True) + 1e-6)
            dot_mean = jnp.mean(da * wide, -1, keepdims=True)
            dwide = scale * da - wide * (scale * scale * scale * dot_mean)
            dy_v[r] = (dy_v[r].astype(f32) + dwide.astype(bf16).astype(f32)).astype(bf16)

        loop(tokens // TILE, tile)

    inner = me + 2 - 4 * lax.div(z, 3)
    is_end = (z == 0) | (z == 3)

    def hand():
        return [
            pltpu.make_async_remote_copy(og.at[1, 1, :, 0:WIDE], og.at[0, 1, :, 0:WIDE], hsend.at[0], hrecv.at[0], device_id={"dp": inner}),
            pltpu.make_async_remote_copy(ou.at[1, 1, :, 0:WIDE], ou.at[0, 1, :, 0:WIDE], hsend.at[1], hrecv.at[1], device_id={"dp": inner}),
            pltpu.make_async_remote_copy(od.at[1, 1, 0:DHALF], od.at[0, 1, 0:DHALF], hsend.at[2], hrecv.at[2], device_id={"dp": inner}),
        ]

    def step(s):
        l, slot, at = 1 - lax.div(s, 4), lax.rem(s, SLOTS), odd(s)
        q, e = quarter(s), 6 * s
        for copy in weights(l, q, at):
            copy.wait()

        @pl.when(s < ITEMS - 1)
        def _():
            for copy in weights(1 - lax.div(s + 1, 4), quarter(s + 1), 1 - at):
                copy.start()

        @pl.when(s == 4)
        def _():
            backward_norm()
            for t in BOTH:
                for copy in fetch(q, t):
                    copy.start()

        def slopes(r, c0, cn, g, u, d):
            sig = sigmoid(g)
            silu = g * sig
            big[r, c0 : c0 + cn] = (d * (u * (sig + silu * (1 - sig)))).astype(bf16)
            to = EDGE + c0 if cn == TILE else D
            big[r, to : to + cn] = (d * silu).astype(bf16)
            return silu

        def tile(t):
            r = rows(t, TM)

            @pl.when(s < 4)
            def _():
                a, dh = a_v[1, r], dy_v[r]
                for c0, cn, g, u in gate_up(a, at):
                    d = dot_bt(dh, wdb_v[at, c0 : c0 + cn]).astype(bf16).astype(f32)
                    silu = slopes(r, c0, cn, g, u, d)
                    big[r, 2 * Q + c0 : 2 * Q + c0 + cn] = (silu * u).astype(bf16)

            @pl.when(s >= 4)
            def _():
                for copy in fetch(q, t):
                    copy.wait()
                b, dh = odd(t), dy_v[r]
                for c0, cn in COLS:
                    d = dot_bt(dh, wdb_v[at, c0 : c0 + cn]).astype(bf16).astype(f32)
                    slopes(r, c0, cn, stage[b, 0:TM, c0 : c0 + cn], stage[b, TM : 2 * TM, c0 : c0 + cn], d)

                @pl.when(s < ITEMS - 1)
                def _():
                    for copy in fetch(quarter(s + 1), t):
                        copy.start()

            engine(e + t)

        loop(2, tile)

        @pl.when(s >= 4)
        def _():
            fetch_act(q).wait()
            settle(s - SLOTS)
            pl.semaphore_wait(pcredit)

        once = 1 + lax.div(s, ITEMS)

        def down_part(_):
            value = dot_at(big[:, 2 * Q : 3 * Q], dy_v[...]).astype(bf16).reshape(2, 2, 2, R, D)
            for h in BOTH:
                for core in BOTH:
                    own[slot, 4:6, core, :, D * h : D * h + D] = value[core, :, h]

        loop(once, down_part)
        swap(s, 0).start()

        @pl.when((s >= 3) & (s < ITEMS - 1))
        def _():
            fetch_act(quarter(s + 1)).start()

        engine(e + 2)

        def gate_part(_):
            own[slot, 0:4, :, :, 0:EDGE] = dot_at(a_v[l], big[:, 0:EDGE]).astype(bf16).reshape(4, 2, R, EDGE)

        loop(once, gate_part)
        swap(s, 1).start()
        engine(e + 3)
        own[slot, 0:4, :, :, EDGE:WIDE] = dot_at(a_v[l], big[:, EDGE:WIDE]).astype(bf16).reshape(4, 2, R, EVEN)
        swap(s, 2).start()
        engine(e + 4)

        @pl.when(s < 4)
        def _():
            def tile(t):
                r = rows(t, TM)
                da_v[r] += dot_bt(big[r, 0 : 2 * Q], wgu_v[at])

            loop(tiles, tile)

        engine(e + 5)

        @pl.when((s >= SLOTS - 1) & (s < ITEMS - 1))
        def _():
            pl.semaphore_signal(pcredit, device_id=partner)

    loop(ITEMS, step)

    def tail(k):
        @pl.when(is_end & (k == HEAD))
        def _():
            for copy in hand():
                copy.start()

        engine(6 * ITEMS + k)

    loop(HEAD + (LAG * 3) // 2, tail)
    loop(SLOTS, lambda k: settle(ITEMS - SLOTS + k))

    @pl.when(is_end)
    def _():
        for copy in hand():
            copy.wait_send()

    @pl.when(jnp.logical_not(is_end))
    def _():
        for copy in hand():
            copy.wait_recv()

    oss[...] = ss_v[...]


def reduce_gradients(x, dy, wg, wu, wd):
    tokens = x.shape[0]
    hbm, vmem, dma = pl.BlockSpec(memory_space=pl.ANY), pl.BlockSpec(memory_space=pltpu.VMEM), pltpu.SemaphoreType.DMA
    regular = pltpu.SemaphoreType.REGULAR
    return pl.pallas_call(
        step_kernel,
        name="step_kernel",
        out_shape=(
            jax.ShapeDtypeStruct((2, LAYERS, R, F), bf16),
            jax.ShapeDtypeStruct((2, LAYERS, R, F), bf16),
            jax.ShapeDtypeStruct((2, LAYERS, DROWS, D), bf16),
            jax.ShapeDtypeStruct((EIGHT, D), f32),
            jax.ShapeDtypeStruct((4, tokens, Q), f32),
            jax.ShapeDtypeStruct((4, tokens, Q), f32),
            jax.ShapeDtypeStruct((4, tokens, Q), bf16),
        ),
        in_specs=[hbm] * 5,
        out_specs=(hbm, hbm, hbm, vmem, hbm, hbm, hbm),
        scratch_shapes=[
            pltpu.VMEM((tokens, D), bf16),
            pltpu.VMEM((2, tokens, D), bf16),
            pltpu.VMEM((tokens, D), bf16),
            pltpu.VMEM((tokens, F), bf16),
            pltpu.VMEM((2, tokens, D), f32),
            pltpu.VMEM((2, D, 2 * Q), bf16),
            pltpu.VMEM((2, Q, D), bf16),
            pltpu.VMEM((F, D), bf16),
            pltpu.VMEM((SLOTS, 6, 2, R, WIDE), bf16),
            pltpu.VMEM((SLOTS, 6, R, WIDE), bf16),
            pltpu.VMEM((2, PACK, R, D), bf16),
            pltpu.VMEM((EIGHT, D), f32),
            dma((3,)),
            dma((2, 4)),
            dma((3, 2)),
            dma((SLOTS, 3)),
            dma((SLOTS, 3)),
            dma((2, SLOTS, EIGHT)),
            dma((2, PACK)),
            dma((SLOTS, 10)),
            dma((3,)),
            dma((3,)),
            regular((2,)),
            regular((2,)),
            regular,
        ],
        compiler_params=pltpu.CompilerParams(collective_id=0, has_side_effects=True, vmem_limit_bytes=67043328),
    )(x, dy, wg, wu, wd)


def gather_kernel(
    ss, eg, eu, ed, wg, wu, wd, mg, mu, md, vg, vu, vd, og, ou, od, fg, fu, fd, sg, su, sd,
    gg, gu, gd, bg, bu, bd, sums, part, fac,
    sum_send, sum_recv, g_recv, g_send, in_sem, z_send, z_recv, p_send, p_recv, own_sem,
):
    me, z, c = place()
    partner = {"dp": me + 1 - 2 * c}
    is_end = (z == 0) | (z == 3)
    inner = me + 2 - 4 * lax.div(z, 3)
    ends, gs, outs = (eg, eu, ed), (gg, gu, gd), (og, ou, od)

    def layer_half(k):
        return 1 - half(k), odd(k)

    def cut(ref, mat, part, lead, first):
        if mat < 2:
            return ref.at[(*lead, pl.ds(pl.multiple_of(first * R, PACK), R), rows(part, WIDE))]
        return ref.at[(*lead, pl.ds(pl.multiple_of(first * DROWS + part * DHALF, 32), DHALF), slice(None))]

    def state(mat):
        n = R if mat < 2 else DROWS
        w = (wg, wu, wd)[mat].at[:, pl.ds(pl.multiple_of(me * n, PACK), n)]
        return (
            pltpu.make_async_copy((mg, mu, md)[mat], (fg, fu, fd)[mat], in_sem.at[mat, 0]),
            pltpu.make_async_copy((vg, vu, vd)[mat], (sg, su, sd)[mat], in_sem.at[mat, 1]),
            pltpu.make_async_copy(w, (bg, bu, bd)[mat], in_sem.at[mat, 2]),
        )

    def own_g(k, mat):
        l, part = layer_half(k)
        return pltpu.make_async_copy(cut(ends[mat], mat, part, (0, l), 0), cut(gs[mat], mat, part, (l,), 0), own_sem.at[k, mat])

    def hand_g(k, mat):
        l, part = layer_half(k)
        return pltpu.make_async_remote_copy(
            cut(ends[mat], mat, part, (1, l), 0), cut(gs[mat], mat, part, (l,), 0), g_send.at[k, mat], g_recv.at[k, mat],
            device_id={"dp": inner},
        )

    def send_sum(k):
        return pltpu.make_async_remote_copy(
            part, sums.at[me], sum_send.at[k], sum_recv.at[me], device_id={"dp": lax.rem(me + k, EIGHT)}
        )

    def get_sum(k):
        of = lax.rem(me + k, EIGHT)
        return pltpu.make_async_remote_copy(part, sums.at[of], sum_send.at[k], sum_recv.at[of], device_id={"dp": of})

    def chunk(k, mat, block):
        l, part = layer_half(k)
        return cut(outs[mat], mat, part, (l,), block)

    def along(way, hop, k, mat, block):
        ref = chunk(k, mat, block)
        return pltpu.make_async_remote_copy(
            ref, ref, z_send.at[way, hop, k, mat], z_recv.at[way, hop, k, mat], device_id={"dp": me + 2 - 4 * way}
        )

    def across(k, mat, block):
        ref = chunk(k, mat, block)
        of = half(block)
        return pltpu.make_async_remote_copy(ref, ref, p_send.at[of, k, mat], p_recv.at[of, k, mat], device_id=partner)

    part[...] = sum(ss[:, LANES * n : LANES * n + LANES] for n in range(5))
    sums[me] = part[...]
    barrier = pltpu.get_barrier_semaphore()
    for k in range(1, EIGHT):
        pl.semaphore_signal(barrier, device_id={"dp": lax.rem(me + k, EIGHT)})
    for mat in KINDS:
        for copy in state(mat):
            copy.start()

    def take(k):
        @pl.when(is_end | (k == 0))
        def _():
            for mat in KINDS:
                own_g(k, mat).start()

    loop(4, take)
    pl.semaphore_wait(barrier, 7)
    for k in range(1, EIGHT):
        send_sum(k).start()

    @pl.when(is_end)
    def _():
        def hand(k):
            for mat in KINDS:
                hand_g(k + 1, mat).start()

        loop(3, hand)

    for k in range(1, EIGHT):
        get_sum(k).wait_recv()
    total = jnp.zeros((EIGHT, LANES), f32)
    for k in range(EIGHT):
        total += sums[k]
    total = jnp.sum(jnp.sum(total, 0, keepdims=True), 1, keepdims=True)
    count = LAYERS * 3 * D * F
    factor = jnp.minimum(1.0, 0.5 * lax.rsqrt(total * (1.0 / count) + 1e-30))
    fac[...] = jnp.broadcast_to(factor, fac.shape)
    for mat in KINDS:
        for copy in state(mat):
            copy.wait()

    def adamw(k):
        l, part = layer_half(k)
        for mat in KINDS:
            @pl.when(is_end | (k == 0))
            def _():
                own_g(k, mat).wait()

            @pl.when(jnp.logical_not(is_end) & (k > 0))
            def _():
                hand_g(k, mat).wait_recv()

            def piece(n):
                if mat < 2:
                    r, col = rows(n, PACK), rows(part, WIDE)
                    to = (l, pl.ds(pl.multiple_of(me * R + n * PACK, PACK), PACK), col)
                else:
                    r, col = pl.ds(pl.multiple_of(part * DHALF + n * 32, 32), 32), slice(None)
                    to = (l, pl.ds(pl.multiple_of(me * DROWS + part * DHALF + n * 32, 32), 32), col)
                g = gs[mat][l, r, col].astype(f32) * fac[0:1, 0:1]
                w = (bg, bu, bd)[mat][l, r, col].astype(f32)
                m = 0.9 * (fg, fu, fd)[mat][l, r, col] + 0.1 * g
                v = 0.95 * (sg, su, sd)[mat][l, r, col] + 0.05 * g * g
                (fg, fu, fd)[mat][l, r, col] = m
                (sg, su, sd)[mat][l, r, col] = v
                outs[mat][to] = (w - 0.02 * (m * lax.rsqrt(v + 1e-8) + 0.1 * w)).astype(bf16)

            loop(5, piece)

            @pl.when(z > 0)
            def _():
                along(1, 0, k, mat, me).start()

            @pl.when(z < 3)
            def _():
                along(0, 0, k, mat, me).start()

            across(k, mat, me).start()

    loop(4, adamw)

    def onward(n):
        hop, k = lax.div(n, 4) + 1, lax.rem(n, 4)
        for mat in KINDS:
            @pl.when(z + hop <= 3)
            def _():
                block = me + 2 * hop
                along(1, hop - 1, k, mat, block).wait_recv()

                @pl.when(z > 0)
                def _():
                    along(1, hop, k, mat, block).start()

                across(k, mat, block).start()

            @pl.when(z - hop >= 0)
            def _():
                block = me - 2 * hop
                along(0, hop - 1, k, mat, block).wait_recv()

                @pl.when(z < 3)
                def _():
                    along(0, hop, k, mat, block).start()

                across(k, mat, block).start()

    loop(12, onward)

    def finish(n):
        of, k = lax.div(n, 4), lax.rem(n, 4)
        for mat in KINDS:
            across(k, mat, 2 * of + c).wait_send()
            across(k, mat, 2 * of + 1 - c).wait_recv()

            @pl.when((of >= z) & (z > 0))
            def _():
                along(1, of - z, k, mat, 2 * of + c).wait_send()

            @pl.when((of <= z) & (z < 3))
            def _():
                along(0, z - of, k, mat, 2 * of + c).wait_send()

    loop(PACK, finish)
    for k in range(1, EIGHT):
        send_sum(k).wait_send()

    @pl.when(is_end)
    def _():
        def hand(k):
            for mat in KINDS:
                hand_g(k + 1, mat).wait_send()

        loop(3, hand)


def gather_weights(ss, g, w, m, v):
    hbm, vmem, dma = pl.BlockSpec(memory_space=pl.ANY), pl.BlockSpec(memory_space=pltpu.VMEM), pltpu.SemaphoreType.DMA
    block = [(LAYERS, R, F), (LAYERS, R, F), (LAYERS, DROWS, D)]
    return pl.pallas_call(
        gather_kernel,
        name="gather_kernel",
        out_shape=(
            pltpu.VMEM((LAYERS, D, F), bf16),
            pltpu.VMEM((LAYERS, D, F), bf16),
            pltpu.VMEM((LAYERS, F, D), bf16),
            *(pltpu.VMEM(s, f32) for s in block),
            *(pltpu.VMEM(s, f32) for s in block),
        ),
        in_specs=[vmem] + [hbm] * 12,
        out_specs=(vmem,) * 9,
        scratch_shapes=[
            *(pltpu.VMEM(s, bf16) for s in block),
            *(pltpu.VMEM(s, bf16) for s in block),
            pltpu.VMEM((EIGHT, EIGHT, LANES), f32),
            pltpu.VMEM((EIGHT, LANES), f32),
            pltpu.VMEM((EIGHT, LANES), f32),
            dma((EIGHT,)),
            dma((EIGHT,)),
            dma((4, 3)),
            dma((4, 3)),
            dma((3, 3)),
            dma((2, 4, 4, 3)),
            dma((2, 4, 4, 3)),
            dma((4, 4, 3)),
            dma((4, 4, 3)),
            dma((4, 3)),
        ],
        compiler_params=pltpu.CompilerParams(collective_id=1, has_side_effects=True, vmem_limit_bytes=PACK << 20),
    )(ss, *(pltpu.with_memory_space_constraint(t, pltpu.HBM) for t in (*g, *w, *m, *v)))


def put_kernel(*refs):
    *arrays, sem = refs
    count = len(arrays) // 2
    copies = [pltpu.make_async_copy(arrays[n], arrays[count + n], sem.at[n]) for n in range(count)]
    for copy in copies:
        copy.start()
    for copy in copies:
        copy.wait()


def put(arrays):
    any_space = pl.BlockSpec(memory_space=pl.ANY)
    arrays = [pltpu.with_memory_space_constraint(a, pltpu.VMEM) for a in arrays]
    return pl.pallas_call(
        put_kernel,
        name="put_kernel",
        out_shape=tuple(pltpu.HBM(a.shape, a.dtype) for a in arrays),
        in_specs=[any_space] * len(arrays),
        out_specs=(any_space,) * len(arrays),
        scratch_shapes=[pltpu.SemaphoreType.DMA((len(arrays),))],
        compiler_params=pltpu.CompilerParams(vmem_limit_bytes=1 << 20),
    )(*arrays)


def solution(mesh):
    def body(x, dy, *arrays):
        w, m, v = arrays[0:3], arrays[3:6], arrays[6:9]
        *ends, ss = reduce_gradients(x[0], dy[0], *w)[0:4]
        return put(gather_weights(ss, ends, w, m, v))

    rep, part = P("rep", None, None), P("rep", "dp", None)
    whole, block = P(None, None, None), P(None, "dp", None)
    seq = P(("rep", "dp"), None, None)
    return jax.shard_map(
        body,
        mesh=mesh,
        in_specs=(seq, seq, *[whole] * 3, *[block] * 6),
        out_specs=(*[rep] * 3, *[part] * 6),
        check_vma=False,
    )
```

```python
import functools

import jax
import jax.numpy as jnp
from jax import lax
from jax.experimental import pallas as pl
from jax.experimental.pallas import tpu as pltpu
from jax.sharding import PartitionSpec as P

f32, bf16 = jnp.float32, jnp.bfloat16
D, F, Q = 640, 2560, 640
LAYERS = 2
R, DROWS, DHALF = 80, 320, 160
WIDE, EVEN, EDGE = 1280, 512, 768
LANES, TILE, PACK, EIGHT = 128, 256, 16, 8
KINDS, BOTH = range(3), range(2)
OTHERS = range(1, EIGHT)
CHUNK = ((R, WIDE), (R, WIDE), (DHALF, D))
HEAD = 3
LAG = 6
ITEMS = 8
SLOTS = 4
TM = 1024
COLS = ((0, TILE), (TILE, TILE), (EVEN, LANES))


def dot(a, b):
    return jnp.dot(a, b, preferred_element_type=f32)


def dot_bt(a, b):
    return lax.dot_general(a, b, (((1,), (1,)), ((), ())), preferred_element_type=f32)


def dot_at(a, b):
    return lax.dot_general(a, b, (((0,), (0,)), ((), ())), preferred_element_type=f32)


def sigmoid(g):
    return 0.5 * jnp.tanh(0.5 * g) + 0.5


def flip(way):
    return 1 - way


def odd(i):
    return lax.rem(i, 2)


def half(i):
    return lax.div(i, 2)


def span(start, n):
    return pl.ds(pl.multiple_of(start, LANES if n % LANES == 0 else PACK), n)


def rows(t, n):
    return pl.ds(pl.multiple_of(t * n, n), n)


def loop(n, body):
    lax.fori_loop(0, n, lambda i, _: (body(i), 0)[1], 0)


def place():
    me = lax.axis_index("dp")
    return me, half(me), odd(me)


def quarter(i):
    r = lax.rem(i, 4)
    o, h = odd(r), half(r)
    return (1 - o) * (2 + h) + o * (1 - h)


def step_kernel(
    x, dy, wg, wu, wd, mg, mu, md, vg, vu, vd,
    og, ou, od, ofac, gate_h, up_h, act_h, emg, emu, emd, evg, evu, evd,
    h_v, a_v, dy_v, big, stage, wgu_v, wdb_v, wda_v, own, pair, got, ss_v, sums, part,
    in_sem, w_sem, save_sem, psend, precv, send_sem, recv_sem, keep_sem, hsend, hrecv, esend, erecv, sum_send, sum_recv, credit, dcredit, pcredit,
):
    tokens = x.shape[0]
    tiles = tokens // TM
    me, z, c = place()
    partner = {"dp": me + 1 - 2 * c}

    def weights(l, q, slot, down=True):
        cols = rows(q, Q)
        first = pl.ds(pl.multiple_of(q * Q, LANES), EVEN)
        last = pl.ds(pl.multiple_of(q * Q + EVEN, LANES), LANES)
        two = (
            pltpu.make_async_copy(wg.at[l, :, cols], wgu_v.at[slot, :, 0:D], w_sem.at[slot, 0]),
            pltpu.make_async_copy(wu.at[l, :, last], wgu_v.at[slot, :, D:EDGE], w_sem.at[slot, 1]),
            pltpu.make_async_copy(wu.at[l, :, first], wgu_v.at[slot, :, EDGE:WIDE], w_sem.at[slot, 2]),
        )
        return two + (pltpu.make_async_copy(wd.at[l, cols], wdb_v.at[slot], w_sem.at[slot, 3]),) if down else two

    da_v = stage.at[0]

    def held(n, t):
        b, at = odd(t), rows(t, TM)
        return [(stage.at[b, k * TM : k * TM + TM], ref.at[n, at], save_sem.at[b, k]) for k, ref in ((0, gate_h), (1, up_h))]

    def save(n, t):
        return [pltpu.make_async_copy(here, there, sem) for here, there, sem in held(n, t)]

    def fetch(n, t):
        return [pltpu.make_async_copy(there, here, sem) for here, there, sem in held(n, t)]

    def save_act(n):
        return pltpu.make_async_copy(big.at[:, rows(n, Q)], act_h.at[n], save_sem.at[2, 0])

    def fetch_act(n):
        return pltpu.make_async_copy(act_h.at[n], big.at[:, 2 * Q : 3 * Q], save_sem.at[2, 1])

    load_x = pltpu.make_async_copy(x, h_v, in_sem.at[0])
    load_dy = pltpu.make_async_copy(dy, dy_v, in_sem.at[1])
    load_wd = pltpu.make_async_copy(wd.at[0], wda_v, in_sem.at[2])
    load_x.start()
    for copy in weights(0, 0, 0, False):
        copy.start()
    load_wd.start()
    load_dy.start()

    ss_v[...] = jnp.zeros_like(ss_v)

    def clear(k):
        for way in BOTH:
            got[way, k] = jnp.zeros((R, D), bf16)

    loop(PACK, clear)
    barrier = pltpu.get_barrier_semaphore()
    for k in OTHERS:
        pl.semaphore_signal(barrier, device_id={"dp": lax.rem(me + k, EIGHT)})
    is_end = (z == 0) | (z == 3)
    is_inner = jnp.logical_not(is_end)

    def early():
        out = []
        for n, (src, dst) in enumerate(zip((mg, mu, md, vg, vu, vd), (emg, emu, emd, evg, evu, evd), strict=True)):
            src = src.at[0, DHALF:DROWS] if n % 3 == 2 else src.at[0, :, WIDE:F]
            out.append(pltpu.make_async_remote_copy(src, dst, esend.at[n], erecv.at[n], device_id={"dp": me + 4 * z - 6}))
        return out

    load_x.wait()

    def norm(l):
        def tile(t):
            r = rows(t, TILE)
            wide = h_v[r].astype(f32)
            a = (wide * lax.rsqrt(jnp.mean(wide * wide, -1, keepdims=True) + 1e-6)).astype(bf16)
            a_v[l, r] = a

        loop(tokens // TILE, tile)

    norm(0)

    def gate_up(a, slot):
        for c0, cn in COLS:
            if cn == TILE:
                yield c0, cn, dot(a, wgu_v[slot, :, c0 : c0 + TILE]), dot(a, wgu_v[slot, :, EDGE + c0 : 1024 + c0])
            else:
                both = dot(a, wgu_v[slot, :, EVEN:EDGE])
                yield c0, cn, both[:, 0:LANES], both[:, LANES:TILE]

    def forward(n):
        slot = odd(n)
        for copy in weights(0, n, slot, False):
            copy.wait()

        @pl.when(n < 3)
        def _():
            for copy in weights(0, n + 1, 1 - slot, False):
                copy.start()

        @pl.when(n == 1)
        def _():
            pl.semaphore_wait(barrier, EIGHT - 1)

            @pl.when(is_inner)
            def _():
                for copy in early():
                    copy.start()

        def tile(t):
            @pl.when((n > 0) | (t >= 2))
            def _():
                for copy in save(n, t):
                    copy.wait()

            r = rows(t, TM)
            b = odd(t)
            a = a_v[0, r]
            for c0, cn, g, u in gate_up(a, slot):
                big[r, pl.ds(pl.multiple_of(n * Q + c0, LANES), cn)] = (g * sigmoid(g) * u).astype(bf16)
                stage[b, 0:TM, c0 : c0 + cn] = g
                stage[b, TM : 2 * TM, c0 : c0 + cn] = u
            for copy in save(n, t):
                copy.start()

        loop(tiles, tile)

        @pl.when(n > 0)
        def _():
            save_act(n - 1).wait()

        save_act(n).start()

    loop(4, forward)
    for copy in weights(1, quarter(0), 0):
        copy.start()
    load_wd.wait()

    def down(t):
        r = rows(t, TM)
        h_v[r] = h_v[r] + dot(big[r], wda_v[...]).astype(bf16)

    loop(tiles, down)
    norm(1)
    for t in (tiles - 2, tiles - 1):
        for copy in save(3, t):
            copy.wait()
    save_act(3).wait()

    def zero(t):
        da_v[rows(t, LANES)] = jnp.zeros((LANES, D), f32)

    loop(tokens // LANES, zero)
    load_dy.wait()
    for copy in fetch(quarter(4), 1):
        copy.start()

    def is_last(way):
        return z == 3 * flip(way)

    def is_first(way):
        return z == 3 * way

    def onward(way):
        return {"dp": me + 2 - 4 * way}

    def half_of(ref, k, h):
        return ref.at[(*k, slice(None), pl.ds(pl.multiple_of(D * h, LANES), D))]

    def send(way, item, k, h, u, g):
        slot = lax.rem(item, SLOTS)
        return pltpu.make_async_remote_copy(
            half_of(own, (slot, k, c), h), got.at[way, g], send_sem.at[way, slot, u], recv_sem.at[way, g], device_id=onward(way)
        )

    def keep(way, item, k, u, kind):
        slot, q, l = lax.rem(item, SLOTS), quarter(item), 1 - lax.div(item, 4)
        if kind == 0:
            j, p = way * q + flip(way) * (3 - q), u - 4
            out = od.at[j, l, pl.ds(pl.multiple_of(p * R, PACK), R)]
            return [pltpu.make_async_copy(half_of(own, (slot, k, c), odd(p)), out, keep_sem.at[slot, u])]
        b = odd(u)
        j = way * b + flip(way) * (1 - b)
        mine, out = own.at[slot, k, c], (og, ou)[kind - 1].at[j, l]
        if kind == 1:
            return [pltpu.make_async_copy(mine.at[:, 0:D], out.at[:, rows(q, Q)], keep_sem.at[slot, u])]
        first = pl.ds(pl.multiple_of(q * Q, LANES), EVEN)
        last = pl.ds(pl.multiple_of(q * Q + EVEN, LANES), LANES)
        return [
            pltpu.make_async_copy(mine.at[:, EDGE:WIDE], out.at[:, first], keep_sem.at[slot, u]),
            pltpu.make_async_copy(mine.at[:, D:EDGE], out.at[:, last], keep_sem.at[slot, 6 + u]),
        ]

    def gu_unit(way, item, u):
        return 2 * flip(way) + odd(u), half(u), odd(item) * 4 + u

    def d_unit(item, p):
        return 4 + half(p), odd(p), EIGHT + odd(half(item)) * 4 + p

    def swap(item, kind):
        slot = lax.rem(item, SLOTS)
        if kind == 0:
            src, dst = own.at[slot, 4:6, 1 - c], pair.at[slot, 4:6]
        else:
            cols = slice(D * (kind - 1), D * kind)
            src, dst = own.at[slot, 0:4, 1 - c, :, cols], pair.at[slot, 0:4, :, cols]
        return pltpu.make_async_remote_copy(src, dst, psend.at[slot, kind], precv.at[slot, kind], device_id=partner)

    def settle(item):
        for kind in KINDS:
            swap(item, kind).wait_send()

        def one(way):
            @pl.when(is_last(way))
            def _():
                for u in range(4):
                    for copy in keep(way, item, gu_unit(way, item, u)[0], u, 1 + u // 2):
                        copy.wait()

                @pl.when(odd(item) == way)
                def _():
                    for p in range(4):
                        for copy in keep(way, item, d_unit(item, p)[0], 4 + p, 0):
                            copy.wait()

            @pl.when(jnp.logical_not(is_last(way)))
            def _():
                for u in range(4):
                    k, h, g = gu_unit(way, item, u)
                    send(way, item, k, h, u, g).wait_send()

                @pl.when(odd(item) == way)
                def _():
                    for p in range(4):
                        k, h, g = d_unit(item, p)
                        send(way, item, k, h, 4 + p, g).wait_send()

        loop(2, one)

    def unit(way, n):
        i, j = lax.div(n, 6), lax.rem(n, 6)
        late = odd(i + way)
        first, last = is_first(way), is_last(way)
        passes = jnp.logical_not(last)
        back = {"dp": me - 2 + 4 * way}

        @pl.when(passes & (i >= 2) & (j == 2))
        def _():
            pl.semaphore_wait(credit.at[way])

        @pl.when(passes & (i >= 4) & (j == 0) & (late == 0))
        def _():
            pl.semaphore_wait(dcredit.at[way])

        is_d = lax.convert_element_type(j < 2, jnp.int32)
        item = i - is_d * late
        some = lax.convert_element_type(item >= 0, jnp.int32)
        more = is_d * (1 - late) * lax.div(i, ITEMS - 1)
        v = lax.max(j - 2, 0)

        def one(x, _):
            p = 2 * late + j + 2 * x
            k, h, g = (is_d * a + (1 - is_d) * b for a, b in zip(d_unit(item, p), gu_unit(way, item, v), strict=True))
            u = is_d * (4 + p) + (1 - is_d) * v
            slot = lax.rem(item, SLOTS)
            mine, other = half_of(own, (slot, k, c), h), half_of(pair, (slot, k), h)

            @pl.when(jnp.logical_not(first))
            def _():
                send(way, item, k, h, u, g).wait_recv()

            total = (mine[...].astype(f32) + other[...].astype(f32) + got[way, g].astype(f32)).astype(bf16)
            mine[...] = total

            @pl.when(passes)
            def _():
                send(way, item, k, h, u, g).start()

            @pl.when(last)
            def _():
                wide = mine[...].astype(f32)
                ss_v[...] += jnp.sum((wide * wide).reshape(10, EIGHT, D), 0)
                for kind in KINDS:
                    @pl.when(half(j) == kind)
                    def _():
                        for copy in keep(way, item, k, u, kind):
                            copy.start()

            return 0

        lax.fori_loop(0, some * (1 + more), one, 0)

        @pl.when(jnp.logical_not(first) & (i < ITEMS - 2) & (j == 5))
        def _():
            pl.semaphore_signal(credit.at[way], device_id=back)

        @pl.when(jnp.logical_not(first) & (late == 1) & (i >= 1) & (i <= 4) & (j == 1))
        def _():
            pl.semaphore_signal(dcredit.at[way], device_id=back)

    upper = half(z)

    def engine(e):
        n = e - HEAD
        for kind in KINDS:
            @pl.when((n >= 0) & (n < 6 * ITEMS) & (lax.rem(n, 6) == 2 * kind))
            def _():
                swap(lax.div(n, 6), kind).wait_recv()

        def one(j):
            way = upper * j + (1 - upper) * (1 - j)
            hops = way * (3 - z) + flip(way) * z
            mine = n - half(LAG * hops)

            @pl.when((mine >= 0) & (mine < 6 * ITEMS))
            def _():
                unit(way, mine)

        loop(2, one)

    def backward_norm():
        def tile(t):
            r = rows(t, TILE)
            wide, da = h_v[r].astype(f32), da_v[r].astype(bf16).astype(f32)
            scale = lax.rsqrt(jnp.mean(wide * wide, -1, keepdims=True) + 1e-6)
            dot_mean = jnp.mean(da * wide, -1, keepdims=True)
            dwide = scale * da - wide * (scale * scale * scale * dot_mean)
            dy_v[r] = (dy_v[r].astype(f32) + dwide.astype(bf16).astype(f32)).astype(bf16)

        loop(tokens // TILE, tile)

    inner = me + 2 - 4 * lax.div(z, 3)
    def hand():
        return [
            pltpu.make_async_remote_copy(og.at[1, 1, :, 0:WIDE], og.at[0, 1, :, 0:WIDE], hsend.at[0], hrecv.at[0], device_id={"dp": inner}),
            pltpu.make_async_remote_copy(ou.at[1, 1, :, 0:WIDE], ou.at[0, 1, :, 0:WIDE], hsend.at[1], hrecv.at[1], device_id={"dp": inner}),
            pltpu.make_async_remote_copy(od.at[1, 1, 0:DHALF], od.at[0, 1, 0:DHALF], hsend.at[2], hrecv.at[2], device_id={"dp": inner}),
        ]

    def step(s):
        l, slot, at = 1 - lax.div(s, 4), lax.rem(s, SLOTS), odd(s)
        q, e = quarter(s), 6 * s
        for copy in weights(l, q, at):
            copy.wait()

        @pl.when(s < ITEMS - 1)
        def _():
            for copy in weights(1 - lax.div(s + 1, 4), quarter(s + 1), 1 - at):
                copy.start()

        @pl.when(s == 4)
        def _():
            backward_norm()
            for copy in fetch(q, 0):
                copy.start()

        def slopes(r, c0, cn, g, u, d):
            sig = sigmoid(g)
            silu = g * sig
            big[r, c0 : c0 + cn] = (d * (u * (sig + silu * (1 - sig)))).astype(bf16)
            to = EDGE + c0 if cn == TILE else D
            big[r, to : to + cn] = (d * silu).astype(bf16)
            return silu

        def tile(turn):
            t = 1 - turn
            r = rows(t, TM)

            @pl.when(s < 4)
            def _():
                a, dh = a_v[1, r], dy_v[r]
                for c0, cn, g, u in gate_up(a, at):
                    d = dot_bt(dh, wdb_v[at, c0 : c0 + cn]).astype(bf16).astype(f32)
                    silu = slopes(r, c0, cn, g, u, d)
                    big[r, 2 * Q + c0 : 2 * Q + c0 + cn] = (silu * u).astype(bf16)

            @pl.when(s >= 4)
            def _():
                for copy in fetch(q, t):
                    copy.wait()
                b, dh = odd(t), dy_v[r]
                for c0, cn in COLS:
                    d = dot_bt(dh, wdb_v[at, c0 : c0 + cn]).astype(bf16).astype(f32)
                    slopes(r, c0, cn, stage[b, 0:TM, c0 : c0 + cn], stage[b, TM : 2 * TM, c0 : c0 + cn], d)

                @pl.when(s < ITEMS - 1)
                def _():
                    for copy in fetch(quarter(s + 1), t):
                        copy.start()

            engine(e + turn)

        loop(2, tile)

        @pl.when(s >= 4)
        def _():
            fetch_act(q).wait()
            settle(s - SLOTS)
            pl.semaphore_wait(pcredit)

        once = 1 + lax.div(s, ITEMS)

        def down_part(_):
            value = dot_at(big[:, 2 * Q : 3 * Q], dy_v[...]).astype(bf16).reshape(2, 2, 2, R, D)
            for h in BOTH:
                for core in BOTH:
                    own[slot, 4:6, core, :, D * h : D * h + D] = value[core, :, h]

        loop(once, down_part)
        swap(s, 0).start()

        @pl.when((s >= 3) & (s < ITEMS - 1))
        def _():
            fetch_act(quarter(s + 1)).start()

        engine(e + 2)

        def gate_part(_):
            own[slot, 0:4, :, :, 0:EDGE] = dot_at(a_v[l], big[:, 0:EDGE]).astype(bf16).reshape(4, 2, R, EDGE)

        loop(once, gate_part)
        swap(s, 1).start()
        engine(e + 3)
        own[slot, 0:4, :, :, EDGE:WIDE] = dot_at(a_v[l], big[:, EDGE:WIDE]).astype(bf16).reshape(4, 2, R, EVEN)
        swap(s, 2).start()
        engine(e + 4)

        @pl.when(s < 4)
        def _():
            def tile(t):
                r = rows(t, TM)
                da_v[r] += dot_bt(big[r, 0 : 2 * Q], wgu_v[at])

            loop(tiles, tile)

        engine(e + 5)

        @pl.when((s >= SLOTS - 1) & (s < ITEMS - 1))
        def _():
            pl.semaphore_signal(pcredit, device_id=partner)

    loop(ITEMS, step)

    def tail(k):
        @pl.when(is_end & (k == HEAD))
        def _():
            for copy in hand():
                copy.start()

        engine(6 * ITEMS + k)

    loop(HEAD + (LAG * 3) // 2, tail)

    def exchange(k, of):
        return pltpu.make_async_remote_copy(
            part, sums.at[of], sum_send.at[k], sum_recv.at[of], device_id={"dp": lax.rem(me + k, EIGHT)}
        )

    part[...] = sum(ss_v[:, LANES * n : LANES * n + LANES] for n in range(5))
    for k in OTHERS:
        exchange(k, me).start()
    sums[me] = part[...]
    loop(SLOTS, lambda k: settle(ITEMS - SLOTS + k))
    for k in OTHERS:
        exchange(k, lax.rem(me + k, EIGHT)).wait_recv()
    total = sum(sums[k] for k in range(EIGHT))
    total = jnp.sum(jnp.sum(total, 0, keepdims=True), 1, keepdims=True)
    count = LAYERS * 3 * D * F
    ofac[...] = jnp.broadcast_to(jnp.minimum(1.0, 0.5 * lax.rsqrt(total * (1.0 / count) + 1e-30)), ofac.shape)

    @pl.when(is_end)
    def _():
        for copy in hand():
            copy.wait_send()
        for copy in early():
            copy.wait_recv()

    @pl.when(is_inner)
    def _():
        for copy in hand():
            copy.wait_recv()
        for copy in early():
            copy.wait_send()

    for k in OTHERS:
        exchange(k, me).wait_send()


def reduce_gradients(x, dy, w, m, v):
    tokens = x.shape[0]
    hbm, vmem, dma = pl.BlockSpec(memory_space=pl.ANY), pl.BlockSpec(memory_space=pltpu.VMEM), pltpu.SemaphoreType.DMA
    regular = pltpu.SemaphoreType.REGULAR
    return pl.pallas_call(
        step_kernel,
        name="step_kernel",
        out_shape=(
            *[jax.ShapeDtypeStruct((2, LAYERS, R, F), bf16)] * 2,
            jax.ShapeDtypeStruct((2, LAYERS, DROWS, D), bf16),
            jax.ShapeDtypeStruct((EIGHT, LANES), f32),
            *[jax.ShapeDtypeStruct((4, tokens, Q), f32)] * 2,
            jax.ShapeDtypeStruct((4, tokens, Q), bf16),
            *(jax.ShapeDtypeStruct(t, f32) for t in CHUNK + CHUNK),
        ),
        in_specs=[hbm] * 11,
        out_specs=(hbm, hbm, hbm, vmem, *[hbm] * 9),
        scratch_shapes=[
            pltpu.VMEM((tokens, D), bf16),
            pltpu.VMEM((2, tokens, D), bf16),
            pltpu.VMEM((tokens, D), bf16),
            pltpu.VMEM((tokens, F), bf16),
            pltpu.VMEM((2, tokens, D), f32),
            pltpu.VMEM((2, D, 2 * Q), bf16),
            pltpu.VMEM((2, Q, D), bf16),
            pltpu.VMEM((F, D), bf16),
            pltpu.VMEM((SLOTS, 6, 2, R, WIDE), bf16),
            pltpu.VMEM((SLOTS, 6, R, WIDE), bf16),
            pltpu.VMEM((2, PACK, R, D), bf16),
            pltpu.VMEM((EIGHT, D), f32),
            pltpu.VMEM((EIGHT, EIGHT, LANES), f32),
            pltpu.VMEM((EIGHT, LANES), f32),
            dma((3,)),
            dma((2, 4)),
            dma((3, 2)),
            dma((SLOTS, 3)),
            dma((SLOTS, 3)),
            dma((2, SLOTS, EIGHT)),
            dma((2, PACK)),
            dma((SLOTS, 10)),
            *[dma((EIGHT,))] * 6,
            regular((2,)),
            regular((2,)),
            regular,
        ],
        compiler_params=pltpu.CompilerParams(collective_id=0, has_side_effects=True, vmem_limit_bytes=67043328),
    )(x, dy, *w, *m, *v)


def gather_kernel(
    ofac, emg, emu, emd, evg, evu, evd, eg, eu, ed, wg, wu, wd, mg, mu, md, vg, vu, vd, og, ou, od, fg, fu, fd, sg, su, sd,
    gg, gu, gd, bg, bu, bd, xmg, xmu, xmd, xvg, xvu, xvd, xgg, xgu, xgd, xwg, xwu, xwd, fac,
    fac_sem, x_sem, g_recv, g_send, in_sem, z_send, z_recv, p_send, p_recv, own_sem,
):
    me, z, c = place()
    partner = {"dp": me + 1 - 2 * c}
    is_end = (z == 0) | (z == 3)
    inner = me + 2 - 4 * lax.div(z, 3)
    ends, gs, outs = (eg, eu, ed), (gg, gu, gd), (og, ou, od)

    def layer_half(k):
        return 1 - half(k), odd(k)

    def cut(ref, mat, part, lead, first):
        if mat < 2:
            return ref.at[(*lead, pl.ds(pl.multiple_of(first * R, PACK), R), rows(part, WIDE))]
        return ref.at[(*lead, pl.ds(pl.multiple_of(first * DROWS + part * DHALF, 32), DHALF), slice(None))]

    def state(mat, l):
        n = R if mat < 2 else DROWS
        w = (wg, wu, wd)[mat].at[l, pl.ds(pl.multiple_of(me * n, PACK), n)]
        sources = ((mg, mu, md)[mat].at[l], (vg, vu, vd)[mat].at[l], w)
        return [
            pltpu.make_async_copy(src, there[mat].at[l], in_sem.at[mat, l, n])
            for n, (src, there) in enumerate(zip(sources, ((fg, fu, fd), (sg, su, sd), (bg, bu, bd)), strict=True))
        ]

    def own_g(k, mat):
        l, part = layer_half(k)
        return pltpu.make_async_copy(cut(ends[mat], mat, part, (0, l), 0), cut(gs[mat], mat, part, (l,), 0), own_sem.at[k, mat])

    def hand_g(k, mat):
        l, part = layer_half(k)
        return pltpu.make_async_remote_copy(
            cut(ends[mat], mat, part, (1, l), 0), cut(gs[mat], mat, part, (l,), 0), g_send.at[k, mat], g_recv.at[k, mat],
            device_id={"dp": inner},
        )

    def outer(mat):
        w = (wg, wu, wd)[mat]
        return (
            pltpu.make_async_copy((emg, emu, emd)[mat], (xmg, xmu, xmd)[mat], x_sem.at[mat, 0]),
            pltpu.make_async_copy((evg, evu, evd)[mat], (xvg, xvu, xvd)[mat], x_sem.at[mat, 1]),
            pltpu.make_async_copy(cut(ends[mat], mat, 1, (1, 0), 0), (xgg, xgu, xgd)[mat], x_sem.at[mat, 2]),
            pltpu.make_async_copy(cut(w, mat, 1, (0,), inner), (xwg, xwu, xwd)[mat], x_sem.at[mat, 3]),
        )

    def chunk(k, mat, block):
        l, part = layer_half(k)
        return cut(outs[mat], mat, part, (l,), block)

    def along(way, hop, k, mat, block):
        ref = chunk(k, mat, block)
        return pltpu.make_async_remote_copy(
            ref, ref, z_send.at[way, hop, k, mat], z_recv.at[way, hop, k, mat], device_id={"dp": me + 2 - 4 * way}
        )

    def across(k, mat, block):
        ref = chunk(k, mat, block)
        of = half(block)
        return pltpu.make_async_remote_copy(ref, ref, p_send.at[of, k, mat], p_recv.at[of, k, mat], device_id=partner)

    barrier = pltpu.get_barrier_semaphore()
    pl.semaphore_signal(barrier, device_id=partner)

    @pl.when(z > 0)
    def _():
        pl.semaphore_signal(barrier, device_id={"dp": me - 2})

    @pl.when(z < 3)
    def _():
        pl.semaphore_signal(barrier, device_id={"dp": me + 2})

    factor = pltpu.make_async_copy(ofac, fac, fac_sem)
    factor.start()

    def load(l):
        for mat in KINDS:
            for copy in state(mat, l):
                copy.start()

    def take(k):
        @pl.when(is_end | (k == 0))
        def _():
            for mat in KINDS:
                own_g(k, mat).start()

    take(0)
    load(1)
    pl.semaphore_wait(barrier, 2 + lax.convert_element_type(jnp.logical_not(is_end), jnp.int32))

    @pl.when(is_end)
    def _():
        for mat in KINDS:
            for copy in outer(mat):
                copy.start()

        def hand(k):
            for mat in KINDS:
                hand_g(k + 1, mat).start()

        loop(3, hand)

    load(0)
    loop(3, lambda k: take(k + 1))
    factor.wait()

    def stepped(g, w, m, v):
        g = g.astype(f32) * fac[0:1, 0:1]
        w = w.astype(f32)
        m = 0.9 * m + 0.1 * g
        v = 0.95 * v + 0.05 * g * g
        return m, v, (w - 0.02 * (m * lax.rsqrt(v + 1e-8) + 0.1 * w)).astype(bf16)

    def crosses(way, k):
        edge, near = 3 * flip(way), 2 - way
        return (z != edge) & ((z != near) | (k < 3))

    def adamw(k):
        l, part = layer_half(k)
        for mat in KINDS:
            @pl.when(part == 0)
            def _():
                for copy in state(mat, l):
                    copy.wait()

            @pl.when(is_end | (k == 0))
            def _():
                own_g(k, mat).wait()

            @pl.when(jnp.logical_not(is_end) & (k > 0))
            def _():
                hand_g(k, mat).wait_recv()

            def piece(n):
                if mat < 2:
                    r, col = rows(n, PACK), rows(part, WIDE)
                    to = (l, pl.ds(pl.multiple_of(me * R + n * PACK, PACK), PACK), col)
                else:
                    r, col = pl.ds(pl.multiple_of(part * DHALF + n * 32, 32), 32), slice(None)
                    to = (l, pl.ds(pl.multiple_of(me * DROWS + part * DHALF + n * 32, 32), 32), col)
                m, v, w = stepped(
                    gs[mat][l, r, col], (bg, bu, bd)[mat][l, r, col], (fg, fu, fd)[mat][l, r, col], (sg, su, sd)[mat][l, r, col]
                )
                (fg, fu, fd)[mat][l, r, col] = m
                (sg, su, sd)[mat][l, r, col] = v
                outs[mat][to] = w

            loop(5, piece)

            for way in (1, 0):
                @pl.when(crosses(way, k))
                def _():
                    along(way, 0, k, mat, me).start()

            across(k, mat, me).start()

    loop(4, adamw)

    @pl.when(is_end)
    def _():
        for mat in KINDS:
            for copy in outer(mat):
                copy.wait()

            def piece(n):
                size = PACK if mat < 2 else 2 * PACK
                r = rows(n, size)
                new = stepped((xgg, xgu, xgd)[mat][r], (xwg, xwu, xwd)[mat][r], (xmg, xmu, xmd)[mat][r], (xvg, xvu, xvd)[mat][r])
                if mat < 2:
                    first, col = inner * R + n * size, slice(WIDE, F)
                else:
                    first, col = inner * DROWS + DHALF + n * size, slice(None)
                outs[mat][0, pl.ds(pl.multiple_of(first, PACK), size), col] = new[2]

            loop(5, piece)
            across(3, mat, inner).start()


    def onward(n):
        hop, k = lax.div(n, 4) + 1, lax.rem(n, 4)
        for mat in KINDS:
            known = (n == 3) & is_end

            @pl.when((z + hop <= 3) & jnp.logical_not(known))
            def _():
                block = me + 2 * hop
                along(1, hop - 1, k, mat, block).wait_recv()

                @pl.when(z > 0)
                def _():
                    along(1, hop, k, mat, block).start()

                across(k, mat, block).start()

            @pl.when((z - hop >= 0) & jnp.logical_not(known))
            def _():
                block = me - 2 * hop
                along(0, hop - 1, k, mat, block).wait_recv()

                @pl.when(z < 3)
                def _():
                    along(0, hop, k, mat, block).start()

                across(k, mat, block).start()

    loop(12, onward)

    def finish(n):
        of, k = lax.div(n, 4), lax.rem(n, 4)
        for mat in KINDS:
            across(k, mat, 2 * of + c).wait_send()
            across(k, mat, 2 * of + 1 - c).wait_recv()

            @pl.when((of > z) & (z > 0) | (of == z) & crosses(1, k))
            def _():
                along(1, of - z, k, mat, 2 * of + c).wait_send()

            @pl.when((of < z) & (z < 3) | (of == z) & crosses(0, k))
            def _():
                along(0, z - of, k, mat, 2 * of + c).wait_send()

    loop(PACK, finish)
    @pl.when(is_end)
    def _():
        def hand(k):
            for mat in KINDS:
                hand_g(k + 1, mat).wait_send()

        loop(3, hand)


def gather_weights(factor, outer, g, w, m, v):
    hbm, vmem, dma = pl.BlockSpec(memory_space=pl.ANY), pl.BlockSpec(memory_space=pltpu.VMEM), pltpu.SemaphoreType.DMA
    block = [(LAYERS, R, F), (LAYERS, R, F), (LAYERS, DROWS, D)]
    return pl.pallas_call(
        gather_kernel,
        name="gather_kernel",
        out_shape=(
            pltpu.VMEM((LAYERS, D, F), bf16),
            pltpu.VMEM((LAYERS, D, F), bf16),
            pltpu.VMEM((LAYERS, F, D), bf16),
            *(pltpu.VMEM(s, f32) for s in block),
            *(pltpu.VMEM(s, f32) for s in block),
        ),
        in_specs=[hbm] * 19,
        out_specs=(vmem,) * 9,
        scratch_shapes=[
            *(pltpu.VMEM(s, bf16) for s in block),
            *(pltpu.VMEM(s, bf16) for s in block),
            *(pltpu.VMEM(s, f32) for s in CHUNK + CHUNK),
            *(pltpu.VMEM(s, bf16) for s in CHUNK + CHUNK),
            pltpu.VMEM((EIGHT, LANES), f32),
            dma,
            dma((3, 4)),
            dma((4, 3)),
            dma((4, 3)),
            dma((3, LAYERS, 3)),
            *[dma((2, 4, 4, 3))] * 2,
            *[dma((4, 4, 3))] * 2,
            dma((4, 3)),
        ],
        compiler_params=pltpu.CompilerParams(collective_id=1, has_side_effects=True, vmem_limit_bytes=24 << 20),
    )(*(pltpu.with_memory_space_constraint(t, pltpu.HBM) for t in (factor, *outer, *g, *w, *m, *v)))


def put_kernel(*refs):
    *arrays, sem = refs
    count = len(arrays) // 2
    copies = [pltpu.make_async_copy(arrays[n], arrays[count + n], sem.at[n]) for n in range(count)]
    for copy in copies:
        copy.start()
    for copy in copies:
        copy.wait()


def put(arrays):
    any_space = pl.BlockSpec(memory_space=pl.ANY)
    arrays = [pltpu.with_memory_space_constraint(a, pltpu.VMEM) for a in arrays]
    return pl.pallas_call(
        put_kernel,
        name="put_kernel",
        out_shape=tuple(pltpu.HBM(a.shape, a.dtype) for a in arrays),
        in_specs=[any_space] * len(arrays),
        out_specs=(any_space,) * len(arrays),
        scratch_shapes=[pltpu.SemaphoreType.DMA((len(arrays),))],
        compiler_params=pltpu.CompilerParams(vmem_limit_bytes=1 << 20),
    )(*arrays)


def solution(mesh):
    def body(x, dy, *arrays):
        w, m, v = arrays[0:3], arrays[3:6], arrays[6:9]
        *ends, factor, _, _, _, a, b, c, d, e, f = reduce_gradients(x[0], dy[0], w, m, v)
        return put(gather_weights(factor, (a, b, c, d, e, f), ends, w, m, v))

    rep, part = P("rep", None, None), P("rep", "dp", None)
    whole, block = P(None, None, None), P(None, "dp", None)
    seq = P(("rep", "dp"), None, None)
    return jax.shard_map(
        body,
        mesh=mesh,
        in_specs=(seq, seq, *[whole] * 3, *[block] * 6),
        out_specs=(*[rep] * 3, *[part] * 6),
        check_vma=False,
    )
```

```python
import functools

import jax
import jax.numpy as jnp
from jax import lax
from jax.experimental import pallas as pl
from jax.experimental.pallas import tpu as pltpu
from jax.sharding import PartitionSpec as P

f32, bf16 = jnp.float32, jnp.bfloat16
D, F, Q = 640, 2560, 640
LAYERS = 2
R, DROWS, DHALF = 80, 320, 160
WIDE, EVEN, EDGE = 1280, 512, 768
LANES, TILE, PACK, EIGHT = 128, 256, 16, 8
KINDS, BOTH = range(3), range(2)
OTHERS = range(1, EIGHT)
CHUNK = ((R, WIDE), (R, WIDE), (DHALF, D))
HEAD = 3
LAG = 3
ITEMS = 8
SLOTS = 4
TM = 1024
COLS = ((0, TILE), (TILE, TILE), (EVEN, LANES))


def dot(a, b):
    return jnp.dot(a, b, preferred_element_type=f32)


def dot_bt(a, b):
    return lax.dot_general(a, b, (((1,), (1,)), ((), ())), preferred_element_type=f32)


def dot_at(a, b):
    return lax.dot_general(a, b, (((0,), (0,)), ((), ())), preferred_element_type=f32)


def sigmoid(g):
    return 0.5 * jnp.tanh(0.5 * g) + 0.5


def flip(way):
    return 1 - way


def odd(i):
    return lax.rem(i, 2)


def half(i):
    return lax.div(i, 2)


def span(start, n):
    return pl.ds(pl.multiple_of(start, LANES if n % LANES == 0 else PACK), n)


def rows(t, n):
    return pl.ds(pl.multiple_of(t * n, n), n)


def loop(n, body):
    lax.fori_loop(0, n, lambda i, _: (body(i), 0)[1], 0)


def place():
    me = lax.axis_index("dp")
    c = odd(me)
    return me, half(me), c, {"dp": me + 1 - 2 * c}


def ahead(me, way):
    return {"dp": me + 2 - 4 * way}


def at_end(z):
    return (z == 0) | (z == 3)


def layer_of(item):
    return 1 - lax.div(item, 4)


def quarter(i):
    r = lax.rem(i, 4)
    o, h = odd(r), half(r)
    return (1 - o) * (2 + h) + o * (1 - h)


def step_kernel(
    x, dy, wg, wu, wd, mg, mu, md, vg, vu, vd,
    og, ou, od, ofac, gate_h, up_h, act_h, emg, emu, emd, evg, evu, evd, ehm, ehv,
    h_v, a_v, dy_v, big, stage, wgu_v, wdb_v, wda_v, own, pair, got, ss_v, sums, part,
    in_sem, w_sem, save_sem, psend, precv, send_sem, recv_sem, keep_sem, hsend, hrecv, esend, erecv, sum_send, sum_recv, credit, dcredit, pcredit,
):
    tokens = x.shape[0]
    tiles = tokens // TM
    me, z, c, partner = place()

    def weights(l, q, slot, down=True):
        cols = rows(q, Q)
        first = pl.ds(pl.multiple_of(q * Q, LANES), EVEN)
        last = pl.ds(pl.multiple_of(q * Q + EVEN, LANES), LANES)
        two = (
            pltpu.make_async_copy(wg.at[l, :, cols], wgu_v.at[slot, :, 0:D], w_sem.at[slot, 0]),
            pltpu.make_async_copy(wu.at[l, :, last], wgu_v.at[slot, :, D:EDGE], w_sem.at[slot, 1]),
            pltpu.make_async_copy(wu.at[l, :, first], wgu_v.at[slot, :, EDGE:WIDE], w_sem.at[slot, 2]),
        )
        return two + (pltpu.make_async_copy(wd.at[l, cols], wdb_v.at[slot], w_sem.at[slot, 3]),) if down else two

    da_v = stage.at[0]

    def held(n, t):
        b, at = odd(t), rows(t, TM)
        return [(stage.at[b, k * TM : k * TM + TM], ref.at[n, at], save_sem.at[b, k]) for k, ref in ((0, gate_h), (1, up_h))]

    def save(n, t):
        return [pltpu.make_async_copy(here, there, sem) for here, there, sem in held(n, t)]

    def fetch(n, t):
        return [pltpu.make_async_copy(there, here, sem) for here, there, sem in held(n, t)]

    def save_act(n):
        return pltpu.make_async_copy(big.at[:, rows(n, Q)], act_h.at[n], save_sem.at[2, 0])

    def fetch_act(n):
        return pltpu.make_async_copy(act_h.at[n], big.at[:, 2 * Q : 3 * Q], save_sem.at[2, 1])

    load_x = pltpu.make_async_copy(x, h_v, in_sem.at[0])
    load_dy = pltpu.make_async_copy(dy, dy_v, in_sem.at[1])
    load_wd = pltpu.make_async_copy(wd.at[0], wda_v, in_sem.at[2])
    load_x.start()
    for copy in weights(0, 0, 0, False):
        copy.start()
    load_wd.start()
    load_dy.start()

    ss_v[...] = jnp.zeros_like(ss_v)

    def clear(k):
        for way in BOTH:
            got[way, k] = jnp.zeros((R, D), bf16)

    loop(PACK, clear)
    barrier = pltpu.get_barrier_semaphore()
    for k in OTHERS:
        pl.semaphore_signal(barrier, device_id={"dp": lax.rem(me + k, EIGHT)})
    is_end = at_end(z)
    is_inner = jnp.logical_not(is_end)

    def early(n, src, dst):
        return pltpu.make_async_remote_copy(src, dst, esend.at[n], erecv.at[n], device_id=ahead(me, 2 - z))

    def early_chunks():
        return [
            early(n, src.at[0, DHALF:DROWS] if n % 3 == 2 else src.at[0, :, WIDE:F], dst)
            for n, (src, dst) in enumerate(zip((mg, mu, md, vg, vu, vd), (emg, emu, emd, evg, evu, evd), strict=True))
        ]

    def early_piece(n, moment):
        at = (rows(half(n), R // 2), rows(odd(n), D))
        return early(6 + 2 * n + moment, (mg, vg)[moment].at[(0, *at)], (ehm, ehv)[moment].at[at])

    load_x.wait()

    def norm(l):
        def tile(t):
            r = rows(t, TILE)
            wide = h_v[r].astype(f32)
            a = (wide * lax.rsqrt(jnp.mean(wide * wide, -1, keepdims=True) + 1e-6)).astype(bf16)
            a_v[l, r] = a

        loop(tokens // TILE, tile)

    norm(0)
    pl.semaphore_wait(barrier, EIGHT - 1)

    @pl.when(is_inner)
    def _():
        for copy in early_chunks():
            copy.start()

    def gate_up(a, slot):
        for c0, cn in COLS:
            if cn == TILE:
                yield c0, cn, dot(a, wgu_v[slot, :, c0 : c0 + TILE]), dot(a, wgu_v[slot, :, EDGE + c0 : 1024 + c0])
            else:
                both = dot(a, wgu_v[slot, :, EVEN:EDGE])
                yield c0, cn, both[:, 0:LANES], both[:, LANES:TILE]

    def forward(n):
        slot = odd(n)
        for copy in weights(0, n, slot, False):
            copy.wait()

        @pl.when(n < 3)
        def _():
            for copy in weights(0, n + 1, 1 - slot, False):
                copy.start()

        def tile(t):
            @pl.when((n > 0) | (t >= 2))
            def _():
                for copy in save(n, t):
                    copy.wait()

            r = rows(t, TM)
            b = odd(t)
            a = a_v[0, r]
            for c0, cn, g, u in gate_up(a, slot):
                big[r, pl.ds(pl.multiple_of(n * Q + c0, LANES), cn)] = (g * sigmoid(g) * u).astype(bf16)
                stage[b, 0:TM, c0 : c0 + cn] = g
                stage[b, TM : 2 * TM, c0 : c0 + cn] = u
            for copy in save(n, t):
                copy.start()

        loop(tiles, tile)

        @pl.when(n > 0)
        def _():
            save_act(n - 1).wait()

        save_act(n).start()

    loop(4, forward)
    for copy in weights(1, quarter(0), 0):
        copy.start()
    load_wd.wait()

    def down(t):
        r = rows(t, TM)
        h_v[r] = h_v[r] + dot(big[r], wda_v[...]).astype(bf16)

    loop(tiles, down)
    norm(1)
    for t in (tiles - 2, tiles - 1):
        for copy in save(3, t):
            copy.wait()
    save_act(3).wait()

    def zero(t):
        da_v[rows(t, LANES)] = jnp.zeros((LANES, D), f32)

    loop(tokens // LANES, zero)
    load_dy.wait()
    for copy in fetch(quarter(4), 1):
        copy.start()

    def is_last(way):
        return z == 3 * flip(way)

    def is_first(way):
        return z == 3 * way

    def half_of(ref, k, h):
        return ref.at[(*k, slice(None), pl.ds(pl.multiple_of(D * h, LANES), D))]

    def send(way, item, k, h, u, g):
        slot = lax.rem(item, SLOTS)
        return pltpu.make_async_remote_copy(
            half_of(own, (slot, k, c), h), got.at[way, g], send_sem.at[way, slot, u], recv_sem.at[way, g], device_id=ahead(me, way)
        )

    def keep(way, item, k, u, kind):
        slot, q, l = lax.rem(item, SLOTS), quarter(item), layer_of(item)
        if kind == 0:
            j, p = way * q + flip(way) * (3 - q), u - 4
            out = od.at[j, l, pl.ds(pl.multiple_of(p * R, PACK), R)]
            return [pltpu.make_async_copy(half_of(own, (slot, k, c), odd(p)), out, keep_sem.at[slot, u])]
        b = odd(u)
        j = way * b + flip(way) * (1 - b)
        mine, out = own.at[slot, k, c], (og, ou)[kind - 1].at[j, l]
        if kind == 1:
            return [pltpu.make_async_copy(mine.at[:, 0:D], out.at[:, rows(q, Q)], keep_sem.at[slot, u])]
        first = pl.ds(pl.multiple_of(q * Q, LANES), EVEN)
        last = pl.ds(pl.multiple_of(q * Q + EVEN, LANES), LANES)
        return [
            pltpu.make_async_copy(mine.at[:, EDGE:WIDE], out.at[:, first], keep_sem.at[slot, u]),
            pltpu.make_async_copy(mine.at[:, D:EDGE], out.at[:, last], keep_sem.at[slot, 6 + u]),
        ]

    def gu_unit(way, item, u):
        return 2 * flip(way) + odd(u), half(u), odd(item) * 4 + u

    def d_unit(item, p):
        return 4 + half(p), odd(p), EIGHT + odd(half(item)) * 4 + p

    def swap(item, kind):
        slot = lax.rem(item, SLOTS)
        if kind == 0:
            src, dst = own.at[slot, 4:6, 1 - c], pair.at[slot, 4:6]
        else:
            cols = slice(D * (kind - 1), D * kind)
            src, dst = own.at[slot, 0:4, 1 - c, :, cols], pair.at[slot, 0:4, :, cols]
        return pltpu.make_async_remote_copy(src, dst, psend.at[slot, kind], precv.at[slot, kind], device_id=partner)

    def settle(item):
        for kind in KINDS:
            swap(item, kind).wait_send()

        def one(way):
            @pl.when(is_last(way))
            def _():
                for u in range(4):
                    for copy in keep(way, item, gu_unit(way, item, u)[0], u, 1 + u // 2):
                        copy.wait()

                @pl.when(odd(item) == way)
                def _():
                    for p in range(4):
                        for copy in keep(way, item, d_unit(item, p)[0], 4 + p, 0):
                            copy.wait()

            @pl.when(jnp.logical_not(is_last(way)))
            def _():
                for u in range(4):
                    k, h, g = gu_unit(way, item, u)
                    send(way, item, k, h, u, g).wait_send()

                @pl.when(odd(item) == way)
                def _():
                    for p in range(4):
                        k, h, g = d_unit(item, p)
                        send(way, item, k, h, 4 + p, g).wait_send()

        loop(2, one)

    def unit(way, n):
        i, j = lax.div(n, 6), lax.rem(n, 6)
        late = odd(i + way)
        first, last = is_first(way), is_last(way)
        passes = jnp.logical_not(last)
        back = ahead(me, flip(way))

        @pl.when(passes & (i >= 2) & (j == 2))
        def _():
            pl.semaphore_wait(credit.at[way])

        @pl.when(passes & (i >= 4) & (j == 0) & (late == 0))
        def _():
            pl.semaphore_wait(dcredit.at[way])

        is_d = lax.convert_element_type(j < 2, jnp.int32)
        item = i - is_d * late
        some = lax.convert_element_type(item >= 0, jnp.int32)
        more = is_d * (1 - late) * lax.div(i, ITEMS - 1)
        v = lax.max(j - 2, 0)

        def one(x, _):
            p = 2 * late + j + 2 * x
            k, h, g = (is_d * a + (1 - is_d) * b for a, b in zip(d_unit(item, p), gu_unit(way, item, v), strict=True))
            u = is_d * (4 + p) + (1 - is_d) * v
            slot = lax.rem(item, SLOTS)
            mine, other = half_of(own, (slot, k, c), h), half_of(pair, (slot, k), h)

            @pl.when(jnp.logical_not(first))
            def _():
                send(way, item, k, h, u, g).wait_recv()

            total = (mine[...].astype(f32) + other[...].astype(f32) + got[way, g].astype(f32)).astype(bf16)
            mine[...] = total

            @pl.when(passes)
            def _():
                send(way, item, k, h, u, g).start()

            @pl.when(last)
            def _():
                wide = mine[...].astype(f32)
                ss_v[...] += jnp.sum((wide * wide).reshape(10, EIGHT, D), 0)
                for kind in KINDS:
                    @pl.when(half(j) == kind)
                    def _():
                        for copy in keep(way, item, k, u, kind):
                            copy.start()

            return 0

        lax.fori_loop(0, some * (1 + more), one, 0)

        @pl.when(jnp.logical_not(first) & (i < ITEMS - 2) & (j == 5))
        def _():
            pl.semaphore_signal(credit.at[way], device_id=back)

        @pl.when(jnp.logical_not(first) & (late == 1) & (i >= 1) & (i <= 4) & (j == 1))
        def _():
            pl.semaphore_signal(dcredit.at[way], device_id=back)

    upper = half(z)

    def engine(e):
        n = e - HEAD
        for kind in KINDS:
            @pl.when((n >= 0) & (n < 6 * ITEMS) & (lax.rem(n, 6) == 2 * kind))
            def _():
                swap(lax.div(n, 6), kind).wait_recv()

        def one(j):
            way = upper * j + (1 - upper) * (1 - j)
            hops = way * (3 - z) + flip(way) * z
            mine = n - LAG * hops

            @pl.when((mine >= 0) & (mine < 6 * ITEMS))
            def _():
                unit(way, mine)

        loop(2, one)

    def backward_norm():
        def tile(t):
            r = rows(t, TILE)
            wide, da = h_v[r].astype(f32), da_v[r].astype(bf16).astype(f32)
            scale = lax.rsqrt(jnp.mean(wide * wide, -1, keepdims=True) + 1e-6)
            dot_mean = jnp.mean(da * wide, -1, keepdims=True)
            dwide = scale * da - wide * (scale * scale * scale * dot_mean)
            dy_v[r] = (dy_v[r].astype(f32) + dwide.astype(bf16).astype(f32)).astype(bf16)

        loop(tokens // TILE, tile)

    inner = ahead(me, lax.div(z, 3))
    def hand():
        return [
            pltpu.make_async_remote_copy(og.at[1, 1, :, 0:WIDE], og.at[0, 1, :, 0:WIDE], hsend.at[0], hrecv.at[0], device_id=inner),
            pltpu.make_async_remote_copy(ou.at[1, 1, :, 0:WIDE], ou.at[0, 1, :, 0:WIDE], hsend.at[1], hrecv.at[1], device_id=inner),
            pltpu.make_async_remote_copy(od.at[1, 1, 0:DHALF], od.at[0, 1, 0:DHALF], hsend.at[2], hrecv.at[2], device_id=inner),
        ]

    def step(s):
        l, slot, at = layer_of(s), lax.rem(s, SLOTS), odd(s)
        q, e = quarter(s), 6 * s
        top = s < 4
        for copy in weights(l, q, at):
            copy.wait()

        @pl.when(s < ITEMS - 1)
        def _():
            for copy in weights(layer_of(s + 1), quarter(s + 1), 1 - at):
                copy.start()

        @pl.when(s == 4)
        def _():
            backward_norm()
            for copy in fetch(q, 0):
                copy.start()

        def slopes(r, c0, cn, g, u, d):
            sig = sigmoid(g)
            silu = g * sig
            big[r, c0 : c0 + cn] = (d * (u * (sig + silu * (1 - sig)))).astype(bf16)
            to = EDGE + c0 if cn == TILE else D
            big[r, to : to + cn] = (d * silu).astype(bf16)
            return silu

        def tile(turn):
            t = 1 - turn
            r = rows(t, TM)

            @pl.when(top)
            def _():
                a, dh = a_v[1, r], dy_v[r]
                for c0, cn, g, u in gate_up(a, at):
                    d = dot_bt(dh, wdb_v[at, c0 : c0 + cn]).astype(bf16).astype(f32)
                    silu = slopes(r, c0, cn, g, u, d)
                    big[r, 2 * Q + c0 : 2 * Q + c0 + cn] = (silu * u).astype(bf16)

            @pl.when(jnp.logical_not(top))
            def _():
                for copy in fetch(q, t):
                    copy.wait()
                b, dh = odd(t), dy_v[r]
                for c0, cn in COLS:
                    d = dot_bt(dh, wdb_v[at, c0 : c0 + cn]).astype(bf16).astype(f32)
                    slopes(r, c0, cn, stage[b, 0:TM, c0 : c0 + cn], stage[b, TM : 2 * TM, c0 : c0 + cn], d)

                @pl.when(s < ITEMS - 1)
                def _():
                    for copy in fetch(quarter(s + 1), t):
                        copy.start()

            for moment in BOTH:
                @pl.when(top & is_inner & (turn == moment))
                def _():
                    early_piece(s, moment).start()

            engine(e + turn)

        loop(2, tile)

        @pl.when(jnp.logical_not(top))
        def _():
            fetch_act(q).wait()
            settle(s - SLOTS)
            pl.semaphore_wait(pcredit)

        once = 1 + lax.div(s, ITEMS)

        def down_part(_):
            value = dot_at(big[:, 2 * Q : 3 * Q], dy_v[...]).astype(bf16).reshape(2, 2, 2, R, D)
            for h in BOTH:
                for core in BOTH:
                    own[slot, 4:6, core, :, D * h : D * h + D] = value[core, :, h]

        loop(once, down_part)
        swap(s, 0).start()

        @pl.when((s >= 3) & (s < ITEMS - 1))
        def _():
            fetch_act(quarter(s + 1)).start()

        engine(e + 2)

        def gate_part(_):
            own[slot, 0:4, :, :, 0:EDGE] = dot_at(a_v[l], big[:, 0:EDGE]).astype(bf16).reshape(4, 2, R, EDGE)

        loop(once, gate_part)
        swap(s, 1).start()
        engine(e + 3)
        own[slot, 0:4, :, :, EDGE:WIDE] = dot_at(a_v[l], big[:, EDGE:WIDE]).astype(bf16).reshape(4, 2, R, EVEN)
        swap(s, 2).start()
        engine(e + 4)

        @pl.when(top)
        def _():
            def tile(t):
                r = rows(t, TM)
                da_v[r] += dot_bt(big[r, 0 : 2 * Q], wgu_v[at])

            loop(tiles, tile)

        engine(e + 5)

        @pl.when((s >= SLOTS - 1) & (s < ITEMS - 1))
        def _():
            pl.semaphore_signal(pcredit, device_id=partner)

    loop(ITEMS, step)

    def tail(k):
        @pl.when(is_end & (k == HEAD))
        def _():
            for copy in hand():
                copy.start()

        engine(6 * ITEMS + k)

    loop(HEAD + 3 * LAG, tail)

    def exchange(k, of):
        return pltpu.make_async_remote_copy(
            part, sums.at[of], sum_send.at[k], sum_recv.at[of], device_id={"dp": lax.rem(me + k, EIGHT)}
        )

    part[...] = sum(ss_v[:, LANES * n : LANES * n + LANES] for n in range(5))
    for k in OTHERS:
        exchange(k, me).start()
    sums[me] = part[...]
    loop(SLOTS, lambda k: settle(ITEMS - SLOTS + k))
    for k in OTHERS:
        exchange(k, lax.rem(me + k, EIGHT)).wait_recv()
    total = sum(sums[k] for k in range(EIGHT))
    total = jnp.sum(jnp.sum(total, 0, keepdims=True), 1, keepdims=True)
    count = LAYERS * 3 * D * F
    ofac[...] = jnp.broadcast_to(jnp.minimum(1.0, 0.5 * lax.rsqrt(total * (1.0 / count) + 1e-30)), ofac.shape)

    @pl.when(is_end)
    def _():
        for copy in hand():
            copy.wait_send()
        for copy in early_chunks():
            copy.wait_recv()
        for n in range(4):
            for moment in BOTH:
                early_piece(n, moment).wait_recv()

    @pl.when(is_inner)
    def _():
        for copy in hand():
            copy.wait_recv()
        for copy in early_chunks():
            copy.wait_send()
        for n in range(4):
            for moment in BOTH:
                early_piece(n, moment).wait_send()

    for k in OTHERS:
        exchange(k, me).wait_send()


def reduce_gradients(x, dy, w, m, v):
    tokens = x.shape[0]
    hbm, vmem, dma = pl.BlockSpec(memory_space=pl.ANY), pl.BlockSpec(memory_space=pltpu.VMEM), pltpu.SemaphoreType.DMA
    regular = pltpu.SemaphoreType.REGULAR
    return pl.pallas_call(
        step_kernel,
        name="step_kernel",
        out_shape=(
            *[jax.ShapeDtypeStruct((2, LAYERS, R, F), bf16)] * 2,
            jax.ShapeDtypeStruct((2, LAYERS, DROWS, D), bf16),
            jax.ShapeDtypeStruct((EIGHT, LANES), f32),
            *[jax.ShapeDtypeStruct((4, tokens, Q), f32)] * 2,
            jax.ShapeDtypeStruct((4, tokens, Q), bf16),
            *(jax.ShapeDtypeStruct(t, f32) for t in (*CHUNK, *CHUNK, *CHUNK[0:2])),
        ),
        in_specs=[hbm] * 11,
        out_specs=(hbm, hbm, hbm, vmem, *[hbm] * 11),
        scratch_shapes=[
            pltpu.VMEM((tokens, D), bf16),
            pltpu.VMEM((2, tokens, D), bf16),
            pltpu.VMEM((tokens, D), bf16),
            pltpu.VMEM((tokens, F), bf16),
            pltpu.VMEM((2, tokens, D), f32),
            pltpu.VMEM((2, D, 2 * Q), bf16),
            pltpu.VMEM((2, Q, D), bf16),
            pltpu.VMEM((F, D), bf16),
            pltpu.VMEM((SLOTS, 6, 2, R, WIDE), bf16),
            pltpu.VMEM((SLOTS, 6, R, WIDE), bf16),
            pltpu.VMEM((2, PACK, R, D), bf16),
            pltpu.VMEM((EIGHT, D), f32),
            pltpu.VMEM((EIGHT, EIGHT, LANES), f32),
            pltpu.VMEM((EIGHT, LANES), f32),
            dma((3,)),
            dma((2, 4)),
            dma((3, 2)),
            dma((SLOTS, 3)),
            dma((SLOTS, 3)),
            dma((2, SLOTS, EIGHT)),
            dma((2, PACK)),
            dma((SLOTS, 10)),
            *[dma((PACK,))] * 6,
            regular((2,)),
            regular((2,)),
            regular,
        ],
        compiler_params=pltpu.CompilerParams(collective_id=0, has_side_effects=True, vmem_limit_bytes=67043328),
    )(x, dy, *w, *m, *v)


def gather_kernel(
    ofac, emg, emu, emd, evg, evu, evd, ehm, ehv, eg, eu, ed, wg, wu, wd, mg, mu, md, vg, vu, vd, og, ou, od, fg, fu, fd, sg, su, sd,
    gg, gu, gd, bg, bu, bd, xmg, xmu, xmd, xmh, xvg, xvu, xvd, xvh, xgg, xgu, xgd, xgh, xwg, xwu, xwd, xwh, fac,
    fac_sem, x_sem, g_recv, g_send, in_sem, z_send, z_recv, p_send, p_recv, own_sem,
):
    me, z, c, partner = place()
    is_end = at_end(z)
    inner = ahead(me, lax.div(z, 3))
    known = 2, 3, 3
    ends, gs, outs = (eg, eu, ed), (gg, gu, gd), (og, ou, od)
    given = (xmg, xmu, xmd, xmh), (xvg, xvu, xvd, xvh), (xgg, xgu, xgd, xgh), (xwg, xwu, xwd, xwh)

    def layer_half(k):
        return 1 - half(k), odd(k)

    def cut(ref, mat, part, lead, first):
        if mat < 2:
            return ref.at[(*lead, pl.ds(pl.multiple_of(first * R, PACK), R), rows(part, WIDE))]
        return ref.at[(*lead, pl.ds(pl.multiple_of(first * DROWS + part * DHALF, 32), DHALF), slice(None))]

    def state(mat, l):
        n = R if mat < 2 else DROWS
        w = (wg, wu, wd)[mat].at[l, pl.ds(pl.multiple_of(me * n, PACK), n)]
        sources = ((mg, mu, md)[mat].at[l], (vg, vu, vd)[mat].at[l], w)
        return [
            pltpu.make_async_copy(src, there[mat].at[l], in_sem.at[mat, l, n])
            for n, (src, there) in enumerate(zip(sources, ((fg, fu, fd), (sg, su, sd), (bg, bu, bd)), strict=True))
        ]

    def own_g(k, mat):
        l, part = layer_half(k)
        return pltpu.make_async_copy(cut(ends[mat], mat, part, (0, l), 0), cut(gs[mat], mat, part, (l,), 0), own_sem.at[k, mat])

    def hand_g(k, mat):
        l, part = layer_half(k)
        return pltpu.make_async_remote_copy(
            cut(ends[mat], mat, part, (1, l), 0), cut(gs[mat], mat, part, (l,), 0), g_send.at[k, mat], g_recv.at[k, mat],
            device_id=inner,
        )

    def outer(x):
        mat, part = (x, 1) if x < 3 else (0, 0)
        sources = (
            (emg, emu, emd, ehm)[x],
            (evg, evu, evd, ehv)[x],
            cut(ends[mat], mat, part, (1, 0), 0),
            cut((wg, wu, wd)[mat], mat, part, (0,), inner["dp"]),
        )
        return [pltpu.make_async_copy(src, there[x], x_sem.at[x, n]) for n, (src, there) in enumerate(zip(sources, given, strict=True))]

    def chunk(k, mat, block):
        l, part = layer_half(k)
        return cut(outs[mat], mat, part, (l,), block)

    def along(way, hop, k, mat, block):
        ref = chunk(k, mat, block)
        return pltpu.make_async_remote_copy(
            ref, ref, z_send.at[way, hop, k, mat], z_recv.at[way, hop, k, mat], device_id=ahead(me, way)
        )

    def across(k, mat, block):
        ref = chunk(k, mat, block)
        of = half(block)
        return pltpu.make_async_remote_copy(ref, ref, p_send.at[of, k, mat], p_recv.at[of, k, mat], device_id=partner)

    barrier = pltpu.get_barrier_semaphore()
    pl.semaphore_signal(barrier, device_id=partner)

    for way in BOTH:
        @pl.when(z != 3 * flip(way))
        def _():
            pl.semaphore_signal(barrier, device_id=ahead(me, way))

    factor = pltpu.make_async_copy(ofac, fac, fac_sem)
    factor.start()

    def load(l):
        for mat in KINDS:
            for copy in state(mat, l):
                copy.start()

    def take(k):
        @pl.when(is_end | (k == 0))
        def _():
            for mat in KINDS:
                own_g(k, mat).start()

    take(0)
    load(1)
    load(0)
    loop(3, lambda k: take(k + 1))
    pl.semaphore_wait(barrier, 2 + lax.convert_element_type(jnp.logical_not(is_end), jnp.int32))

    @pl.when(is_end)
    def _():
        for x in range(4):
            for copy in outer(x):
                copy.start()

        def hand(k):
            for mat in KINDS:
                hand_g(k + 1, mat).start()

        loop(3, hand)

    factor.wait()

    def stepped(g, w, m, v):
        g = g.astype(f32) * fac[0:1, 0:1]
        w = w.astype(f32)
        m = 0.9 * m + 0.1 * g
        v = 0.95 * v + 0.05 * g * g
        return m, v, (w - 0.02 * (m * lax.rsqrt(v + 1e-8) + 0.1 * w)).astype(bf16)

    def crosses(way, k, mat):
        edge, near = 3 * flip(way), 2 - way
        return (z != edge) & ((z != near) | (k < known[mat]))

    upper = half(z)

    def relay(turn, m, mat):
        way = upper * turn + flip(upper) * flip(turn)
        hop, k = lax.div(m, 4) + 1, lax.rem(m, 4)
        of = z + hop * (2 * way - 1)
        block = 2 * of + c

        @pl.when((m >= 0) & (m < 12) & (of >= 0) & (of < 4) & ((m >= 4) | (m < known[mat]) | jnp.logical_not(is_end)))
        def _():
            along(way, hop - 1, k, mat, block).wait_recv()

            @pl.when(z != 3 * flip(way))
            def _():
                along(way, hop, k, mat, block).start()

            across(k, mat, block).start()

    def adamw(k):
        l, part = layer_half(k)
        for mat in KINDS:
            relay(0, k - 2, mat)

            @pl.when(part == 0)
            def _():
                for copy in state(mat, l):
                    copy.wait()

            @pl.when(is_end | (k == 0))
            def _():
                own_g(k, mat).wait()

            @pl.when(jnp.logical_not(is_end) & (k > 0))
            def _():
                hand_g(k, mat).wait_recv()

            def piece(n):
                if mat < 2:
                    r, col = rows(n, PACK), rows(part, WIDE)
                    to = (l, pl.ds(pl.multiple_of(me * R + n * PACK, PACK), PACK), col)
                else:
                    r, col = pl.ds(pl.multiple_of(part * DHALF + n * 32, 32), 32), slice(None)
                    to = (l, pl.ds(pl.multiple_of(me * DROWS + part * DHALF + n * 32, 32), 32), col)
                m, v, w = stepped(
                    gs[mat][l, r, col], (bg, bu, bd)[mat][l, r, col], (fg, fu, fd)[mat][l, r, col], (sg, su, sd)[mat][l, r, col]
                )
                (fg, fu, fd)[mat][l, r, col] = m
                (sg, su, sd)[mat][l, r, col] = v
                outs[mat][to] = w

            loop(5, piece)

            for way in (1, 0):
                @pl.when(crosses(way, k, mat))
                def _():
                    along(way, 0, k, mat, me).start()

            across(k, mat, me).start()

    loop(4, adamw)

    @pl.when(is_end)
    def _():
        for x in range(4):
            for copy in outer(x):
                copy.wait()
            mat, part = (x, 1) if x < 3 else (0, 0)

            def piece(n):
                size = PACK if mat < 2 else 2 * PACK
                r = rows(n, size)
                m, v, g, w = (ref[x][r] for ref in given)
                first = inner["dp"] * (R if mat < 2 else DROWS) + n * size + (0 if mat < 2 else DHALF)
                col = slice(WIDE * part, WIDE * part + WIDE) if mat < 2 else slice(None)
                outs[mat][0, pl.ds(pl.multiple_of(first, PACK), size), col] = stepped(g, w, m, v)[2]

            loop(5, piece)
            across(2 + part, mat, inner["dp"]).start()

    def onward(n):
        for mat in KINDS:
            loop(2, lambda turn: relay(turn, n + 2 - 3 * turn, mat))

    loop(13, onward)

    def finish(n):
        of, k = lax.div(n, 4), lax.rem(n, 4)
        for mat in KINDS:
            across(k, mat, 2 * of + c).wait_send()
            across(k, mat, 2 * of + 1 - c).wait_recv()

            @pl.when((of > z) & (z > 0) | (of == z) & crosses(1, k, mat))
            def _():
                along(1, of - z, k, mat, 2 * of + c).wait_send()

            @pl.when((of < z) & (z < 3) | (of == z) & crosses(0, k, mat))
            def _():
                along(0, z - of, k, mat, 2 * of + c).wait_send()

    loop(PACK, finish)
    @pl.when(is_end)
    def _():
        def hand(k):
            for mat in KINDS:
                hand_g(k + 1, mat).wait_send()

        loop(3, hand)


def gather_weights(factor, outer, g, w, m, v):
    hbm, vmem, dma = pl.BlockSpec(memory_space=pl.ANY), pl.BlockSpec(memory_space=pltpu.VMEM), pltpu.SemaphoreType.DMA
    block = [(LAYERS, R, F), (LAYERS, R, F), (LAYERS, DROWS, D)]
    return pl.pallas_call(
        gather_kernel,
        name="gather_kernel",
        out_shape=(
            pltpu.VMEM((LAYERS, D, F), bf16),
            pltpu.VMEM((LAYERS, D, F), bf16),
            pltpu.VMEM((LAYERS, F, D), bf16),
            *(pltpu.VMEM(s, f32) for s in block),
            *(pltpu.VMEM(s, f32) for s in block),
        ),
        in_specs=[hbm] * 21,
        out_specs=(vmem,) * 9,
        scratch_shapes=[
            *(pltpu.VMEM(s, bf16) for s in block),
            *(pltpu.VMEM(s, bf16) for s in block),
            *(pltpu.VMEM(s, t) for t in (f32, f32, bf16, bf16) for s in (*CHUNK, CHUNK[0])),
            pltpu.VMEM((EIGHT, LANES), f32),
            dma,
            dma((4, 4)),
            dma((4, 3)),
            dma((4, 3)),
            dma((3, LAYERS, 3)),
            *[dma((2, 4, 4, 3))] * 2,
            *[dma((4, 4, 3))] * 2,
            dma((4, 3)),
        ],
        compiler_params=pltpu.CompilerParams(collective_id=1, has_side_effects=True, vmem_limit_bytes=24 << 20),
    )(*(pltpu.with_memory_space_constraint(t, pltpu.HBM) for t in (factor, *outer, *g, *w, *m, *v)))


def put_kernel(*refs):
    *arrays, sem = refs
    count = len(arrays) // 2
    copies = [pltpu.make_async_copy(arrays[n].at[l], arrays[count + n].at[l], sem.at[n, l]) for n in range(count) for l in range(LAYERS)]
    for copy in copies:
        copy.start()
    for copy in copies:
        copy.wait()


def put(arrays):
    any_space = pl.BlockSpec(memory_space=pl.ANY)
    arrays = [pltpu.with_memory_space_constraint(a, pltpu.VMEM) for a in arrays]
    return pl.pallas_call(
        put_kernel,
        name="put_kernel",
        out_shape=tuple(pltpu.HBM(a.shape, a.dtype) for a in arrays),
        in_specs=[any_space] * len(arrays),
        out_specs=(any_space,) * len(arrays),
        scratch_shapes=[pltpu.SemaphoreType.DMA((len(arrays), LAYERS))],
        compiler_params=pltpu.CompilerParams(vmem_limit_bytes=1 << 20),
    )(*arrays)


def solution(mesh):
    def body(x, dy, *arrays):
        w, m, v = arrays[0:3], arrays[3:6], arrays[6:9]
        results = reduce_gradients(x[0], dy[0], w, m, v)
        return put(gather_weights(results[3], results[7:], results[0:3], w, m, v))

    rep, part = P("rep", None, None), P("rep", "dp", None)
    whole, block = P(None, None, None), P(None, "dp", None)
    seq = P(("rep", "dp"), None, None)
    return jax.shard_map(
        body,
        mesh=mesh,
        in_specs=(seq, seq, *[whole] * 3, *[block] * 6),
        out_specs=(*[rep] * 3, *[part] * 6),
        check_vma=False,
    )
```

```python
import functools

import jax
import jax.numpy as jnp
from jax import lax
from jax.experimental import pallas as pl
from jax.experimental.pallas import tpu as pltpu
from jax.sharding import PartitionSpec as P

f32, bf16 = jnp.float32, jnp.bfloat16
D, F, Q = 640, 2560, 640
LAYERS = 2
R, DROWS, DHALF = 80, 320, 160
WIDE, EVEN, EDGE = 1280, 512, 768
LANES, TILE, PACK, EIGHT = 128, 256, 16, 8
KINDS, BOTH = range(3), range(2)
OTHERS = range(1, EIGHT)
CHUNK = ((R, WIDE), (R, WIDE), (DHALF, D))
HEAD = 3
LAG = 3
ITEMS = 8
SLOTS = 4
TM = 1024
COLS = ((0, TILE), (TILE, TILE), (EVEN, LANES))


def dot(a, b):
    return jnp.dot(a, b, preferred_element_type=f32)


def dot_bt(a, b):
    return lax.dot_general(a, b, (((1,), (1,)), ((), ())), preferred_element_type=f32)


def dot_at(a, b):
    return lax.dot_general(a, b, (((0,), (0,)), ((), ())), preferred_element_type=f32)


def sigmoid(g):
    return 0.5 * jnp.tanh(0.5 * g) + 0.5


def flip(way):
    return 1 - way


def odd(i):
    return lax.rem(i, 2)


def half(i):
    return lax.div(i, 2)


def span(start, n):
    return pl.ds(pl.multiple_of(start, LANES if n % LANES == 0 else PACK), n)


def rows(t, n):
    return pl.ds(pl.multiple_of(t * n, n), n)


def loop(n, body):
    lax.fori_loop(0, n, lambda i, _: (body(i), 0)[1], 0)


def place():
    me = lax.axis_index("dp")
    c = odd(me)
    return me, half(me), c, {"dp": me + 1 - 2 * c}


def ahead(me, way):
    return {"dp": me + 2 - 4 * way}


def at_end(z):
    return (z == 0) | (z == 3)


def split(n):
    return lax.div(n, 4), lax.rem(n, 4)


def layer_of(item):
    return 1 - lax.div(item, 4)


def quarter(i):
    r = lax.rem(i, 4)
    o, h = odd(r), half(r)
    return (1 - o) * (2 + h) + o * (1 - h)


def step_kernel(
    x, dy, wg, wu, wd, mg, mu, md, vg, vu, vd,
    og, ou, od, ofac, gate_h, up_h, act_h, emg, emu, emd, evg, evu, evd, ehm, ehv,
    h_v, a_v, dy_v, big, stage, wgu_v, wdb_v, wda_v, own, pair, got, ss_v, sums, part,
    in_sem, w_sem, save_sem, psend, precv, send_sem, recv_sem, keep_sem, hsend, hrecv, esend, erecv, sum_send, sum_recv, credit, dcredit, pcredit,
):
    tokens = x.shape[0]
    tiles = tokens // TM
    me, z, c, partner = place()

    def weights(l, q, slot, down=True):
        cols = rows(q, Q)
        first = pl.ds(pl.multiple_of(q * Q, LANES), EVEN)
        last = pl.ds(pl.multiple_of(q * Q + EVEN, LANES), LANES)
        two = (
            pltpu.make_async_copy(wg.at[l, :, cols], wgu_v.at[slot, :, 0:D], w_sem.at[slot, 0]),
            pltpu.make_async_copy(wu.at[l, :, last], wgu_v.at[slot, :, D:EDGE], w_sem.at[slot, 1]),
            pltpu.make_async_copy(wu.at[l, :, first], wgu_v.at[slot, :, EDGE:WIDE], w_sem.at[slot, 2]),
        )
        return two + (pltpu.make_async_copy(wd.at[l, cols], wdb_v.at[slot], w_sem.at[slot, 3]),) if down else two

    da_v = stage.at[0]

    def held(n, t):
        b, at = odd(t), rows(t, TM)
        return [(stage.at[b, k * TM : k * TM + TM], ref.at[n, at], save_sem.at[b, k]) for k, ref in ((0, gate_h), (1, up_h))]

    def save(n, t):
        return [pltpu.make_async_copy(here, there, sem) for here, there, sem in held(n, t)]

    def fetch(n, t):
        return [pltpu.make_async_copy(there, here, sem) for here, there, sem in held(n, t)]

    def save_act(n):
        return pltpu.make_async_copy(big.at[:, rows(n, Q)], act_h.at[n], save_sem.at[2, 0])

    def fetch_act(n):
        return pltpu.make_async_copy(act_h.at[n], big.at[:, 2 * Q : 3 * Q], save_sem.at[2, 1])

    load_x = [pltpu.make_async_copy(x.at[rows(n, TM)], h_v.at[rows(n, TM)], in_sem.at[2 + n]) for n in BOTH]
    load_dy = pltpu.make_async_copy(dy, dy_v, in_sem.at[1])
    load_wd = pltpu.make_async_copy(wd.at[0], wda_v, in_sem.at[0])
    for copy in load_x:
        copy.start()
    for copy in weights(0, 0, 0, False):
        copy.start()
    load_wd.start()
    load_dy.start()

    ss_v[...] = jnp.zeros_like(ss_v)

    def clear(k):
        for way in BOTH:
            got[way, k] = jnp.zeros((R, D), bf16)

    loop(PACK, clear)
    barrier = pltpu.get_barrier_semaphore()
    for k in OTHERS:
        pl.semaphore_signal(barrier, device_id={"dp": lax.rem(me + k, EIGHT)})
    is_end = at_end(z)
    is_inner = jnp.logical_not(is_end)

    def early(n, src, dst):
        return pltpu.make_async_remote_copy(src, dst, esend.at[n], erecv.at[n], device_id=ahead(me, 2 - z))

    def early_chunks():
        return [
            early(n, src.at[0, DHALF:DROWS] if n % 3 == 2 else src.at[0, :, WIDE:F], dst)
            for n, (src, dst) in enumerate(zip((mg, mu, md, vg, vu, vd), (emg, emu, emd, evg, evu, evd), strict=True))
        ]

    def early_piece(n, moment):
        at = (rows(half(n), R // 2), rows(odd(n), D))
        return early(6 + 2 * n + moment, (mg, vg)[moment].at[(0, *at)], (ehm, ehv)[moment].at[at])

    def norm(l, n):
        def tile(t):
            r = rows(n * (TM // TILE) + t, TILE)
            wide = h_v[r].astype(f32)
            a_v[l, r] = (wide * lax.rsqrt(jnp.mean(wide * wide, -1, keepdims=True) + 1e-6)).astype(bf16)

        loop(TM // TILE, tile)

    for n, copy in enumerate(load_x):
        copy.wait()
        norm(0, n)
    pl.semaphore_wait(barrier, EIGHT - 1)

    @pl.when(is_inner)
    def _():
        for copy in early_chunks():
            copy.start()

    def gate_up(a, slot):
        for c0, cn in COLS:
            if cn == TILE:
                yield c0, cn, dot(a, wgu_v[slot, :, c0 : c0 + TILE]), dot(a, wgu_v[slot, :, EDGE + c0 : 1024 + c0])
            else:
                both = dot(a, wgu_v[slot, :, EVEN:EDGE])
                yield c0, cn, both[:, 0:LANES], both[:, LANES:TILE]

    def forward(n):
        slot = odd(n)
        for copy in weights(0, n, slot, False):
            copy.wait()

        @pl.when(n < 3)
        def _():
            for copy in weights(0, n + 1, 1 - slot, False):
                copy.start()

        def tile(t):
            @pl.when((n > 0) | (t >= 2))
            def _():
                for copy in save(n, t):
                    copy.wait()

            r = rows(t, TM)
            b = odd(t)
            a = a_v[0, r]
            for c0, cn, g, u in gate_up(a, slot):
                big[r, pl.ds(pl.multiple_of(n * Q + c0, LANES), cn)] = (g * sigmoid(g) * u).astype(bf16)
                stage[b, 0:TM, c0 : c0 + cn] = g
                stage[b, TM : 2 * TM, c0 : c0 + cn] = u
            for copy in save(n, t):
                copy.start()

        loop(tiles, tile)

        @pl.when(n > 0)
        def _():
            save_act(n - 1).wait()

        save_act(n).start()

    loop(4, forward)
    for copy in weights(1, quarter(0), 0):
        copy.start()
    load_wd.wait()

    def down(t):
        r = rows(t, TM)
        h_v[r] = h_v[r] + dot(big[r], wda_v[...]).astype(bf16)

    loop(tiles, down)
    loop(2, lambda n: norm(1, n))
    for t in (tiles - 2, tiles - 1):
        for copy in save(3, t):
            copy.wait()
    save_act(3).wait()

    def zero(t):
        da_v[rows(t, LANES)] = jnp.zeros((LANES, D), f32)

    loop(tokens // LANES, zero)
    load_dy.wait()
    for copy in fetch(quarter(4), 1):
        copy.start()

    def is_last(way):
        return z == 3 * flip(way)

    def is_first(way):
        return z == 3 * way

    def half_of(ref, k, h):
        return ref.at[(*k, slice(None), pl.ds(pl.multiple_of(D * h, LANES), D))]

    def send(way, item, k, h, u, g):
        slot = lax.rem(item, SLOTS)
        return pltpu.make_async_remote_copy(
            half_of(own, (slot, k, c), h), got.at[way, g], send_sem.at[way, slot, u], recv_sem.at[way, g], device_id=ahead(me, way)
        )

    def keep(way, item, k, u, kind):
        slot, q, l = lax.rem(item, SLOTS), quarter(item), layer_of(item)
        if kind == 0:
            j, p = way * q + flip(way) * (3 - q), u - 4
            out = od.at[j, l, pl.ds(pl.multiple_of(p * R, PACK), R)]
            return [pltpu.make_async_copy(half_of(own, (slot, k, c), odd(p)), out, keep_sem.at[slot, u])]
        b = odd(u)
        j = way * b + flip(way) * (1 - b)
        mine, out = own.at[slot, k, c], (og, ou)[kind - 1].at[j, l]
        if kind == 1:
            return [pltpu.make_async_copy(mine.at[:, 0:D], out.at[:, rows(q, Q)], keep_sem.at[slot, u])]
        first = pl.ds(pl.multiple_of(q * Q, LANES), EVEN)
        last = pl.ds(pl.multiple_of(q * Q + EVEN, LANES), LANES)
        return [
            pltpu.make_async_copy(mine.at[:, EDGE:WIDE], out.at[:, first], keep_sem.at[slot, u]),
            pltpu.make_async_copy(mine.at[:, D:EDGE], out.at[:, last], keep_sem.at[slot, 6 + u]),
        ]

    def gu_unit(way, item, u):
        return 2 * flip(way) + odd(u), half(u), odd(item) * 4 + u

    def d_unit(item, p):
        return 4 + half(p), odd(p), EIGHT + odd(half(item)) * 4 + p

    def swap(item, kind):
        slot = lax.rem(item, SLOTS)
        if kind == 0:
            src, dst = own.at[slot, 4:6, 1 - c], pair.at[slot, 4:6]
        else:
            cols = slice(D * (kind - 1), D * kind)
            src, dst = own.at[slot, 0:4, 1 - c, :, cols], pair.at[slot, 0:4, :, cols]
        return pltpu.make_async_remote_copy(src, dst, psend.at[slot, kind], precv.at[slot, kind], device_id=partner)

    def settle(item):
        for kind in KINDS:
            swap(item, kind).wait_send()

        def one(way):
            @pl.when(is_last(way))
            def _():
                for u in range(4):
                    for copy in keep(way, item, gu_unit(way, item, u)[0], u, 1 + u // 2):
                        copy.wait()

                @pl.when(odd(item) == way)
                def _():
                    for p in range(4):
                        for copy in keep(way, item, d_unit(item, p)[0], 4 + p, 0):
                            copy.wait()

            @pl.when(jnp.logical_not(is_last(way)))
            def _():
                for u in range(4):
                    k, h, g = gu_unit(way, item, u)
                    send(way, item, k, h, u, g).wait_send()

                @pl.when(odd(item) == way)
                def _():
                    for p in range(4):
                        k, h, g = d_unit(item, p)
                        send(way, item, k, h, 4 + p, g).wait_send()

        loop(2, one)

    def unit(way, n):
        i, j = lax.div(n, 6), lax.rem(n, 6)
        late = odd(i + way)
        first, last = is_first(way), is_last(way)
        passes = jnp.logical_not(last)
        back = ahead(me, flip(way))

        @pl.when(passes & (i >= 2) & (j == 2))
        def _():
            pl.semaphore_wait(credit.at[way])

        @pl.when(passes & (i >= 4) & (j == 0) & (late == 0))
        def _():
            pl.semaphore_wait(dcredit.at[way])

        is_d = lax.convert_element_type(j < 2, jnp.int32)
        item = i - is_d * late
        some = lax.convert_element_type(item >= 0, jnp.int32)
        more = is_d * (1 - late) * lax.div(i, ITEMS - 1)
        v = lax.max(j - 2, 0)

        def one(x, _):
            p = 2 * late + j + 2 * x
            k, h, g = (is_d * a + (1 - is_d) * b for a, b in zip(d_unit(item, p), gu_unit(way, item, v), strict=True))
            u = is_d * (4 + p) + (1 - is_d) * v
            slot = lax.rem(item, SLOTS)
            mine, other = half_of(own, (slot, k, c), h), half_of(pair, (slot, k), h)

            @pl.when(jnp.logical_not(first))
            def _():
                send(way, item, k, h, u, g).wait_recv()

            total = (mine[...].astype(f32) + other[...].astype(f32) + got[way, g].astype(f32)).astype(bf16)
            mine[...] = total

            @pl.when(passes)
            def _():
                send(way, item, k, h, u, g).start()

            @pl.when(last)
            def _():
                wide = mine[...].astype(f32)
                ss_v[...] += jnp.sum((wide * wide).reshape(10, EIGHT, D), 0)
                for kind in KINDS:
                    @pl.when(half(j) == kind)
                    def _():
                        for copy in keep(way, item, k, u, kind):
                            copy.start()

            return 0

        lax.fori_loop(0, some * (1 + more), one, 0)

        @pl.when(jnp.logical_not(first) & (i < ITEMS - 2) & (j == 5))
        def _():
            pl.semaphore_signal(credit.at[way], device_id=back)

        @pl.when(jnp.logical_not(first) & (late == 1) & (i >= 1) & (i <= 4) & (j == 1))
        def _():
            pl.semaphore_signal(dcredit.at[way], device_id=back)

    upper = half(z)

    def engine(e):
        n = e - HEAD
        for kind in KINDS:
            @pl.when((n >= 0) & (n < 6 * ITEMS) & (lax.rem(n, 6) == 2 * kind))
            def _():
                swap(lax.div(n, 6), kind).wait_recv()

        def one(j):
            way = upper * j + (1 - upper) * (1 - j)
            hops = way * (3 - z) + flip(way) * z
            mine = n - LAG * hops

            @pl.when((mine >= 0) & (mine < 6 * ITEMS))
            def _():
                unit(way, mine)

        loop(2, one)

    def backward_norm():
        def tile(t):
            r = rows(t, TILE)
            wide, da = h_v[r].astype(f32), da_v[r].astype(bf16).astype(f32)
            scale = lax.rsqrt(jnp.mean(wide * wide, -1, keepdims=True) + 1e-6)
            dot_mean = jnp.mean(da * wide, -1, keepdims=True)
            dwide = scale * da - wide * (scale * scale * scale * dot_mean)
            dy_v[r] = (dy_v[r].astype(f32) + dwide.astype(bf16).astype(f32)).astype(bf16)

        loop(tokens // TILE, tile)

    inner = ahead(me, lax.div(z, 3))
    def hand():
        return [
            pltpu.make_async_remote_copy(og.at[1, 1, :, 0:WIDE], og.at[0, 1, :, 0:WIDE], hsend.at[0], hrecv.at[0], device_id=inner),
            pltpu.make_async_remote_copy(ou.at[1, 1, :, 0:WIDE], ou.at[0, 1, :, 0:WIDE], hsend.at[1], hrecv.at[1], device_id=inner),
            pltpu.make_async_remote_copy(od.at[1, 1, 0:DHALF], od.at[0, 1, 0:DHALF], hsend.at[2], hrecv.at[2], device_id=inner),
        ]

    def step(s):
        l, slot, at = layer_of(s), lax.rem(s, SLOTS), odd(s)
        q, e = quarter(s), 6 * s
        top = s < 4
        for copy in weights(l, q, at):
            copy.wait()

        @pl.when(s < ITEMS - 1)
        def _():
            for copy in weights(layer_of(s + 1), quarter(s + 1), 1 - at):
                copy.start()

        @pl.when(s == 4)
        def _():
            backward_norm()
            for copy in fetch(q, 0):
                copy.start()

        def slopes(r, c0, cn, g, u, d):
            sig = sigmoid(g)
            silu = g * sig
            big[r, c0 : c0 + cn] = (d * (u * (sig + silu * (1 - sig)))).astype(bf16)
            to = EDGE + c0 if cn == TILE else D
            big[r, to : to + cn] = (d * silu).astype(bf16)
            return silu

        def tile(turn):
            t = 1 - turn
            r = rows(t, TM)

            @pl.when(top)
            def _():
                a, dh = a_v[1, r], dy_v[r]
                for c0, cn, g, u in gate_up(a, at):
                    d = dot_bt(dh, wdb_v[at, c0 : c0 + cn]).astype(bf16).astype(f32)
                    silu = slopes(r, c0, cn, g, u, d)
                    big[r, 2 * Q + c0 : 2 * Q + c0 + cn] = (silu * u).astype(bf16)

            @pl.when(jnp.logical_not(top))
            def _():
                for copy in fetch(q, t):
                    copy.wait()
                b, dh = odd(t), dy_v[r]
                for c0, cn in COLS:
                    d = dot_bt(dh, wdb_v[at, c0 : c0 + cn]).astype(bf16).astype(f32)
                    slopes(r, c0, cn, stage[b, 0:TM, c0 : c0 + cn], stage[b, TM : 2 * TM, c0 : c0 + cn], d)

                @pl.when(s < ITEMS - 1)
                def _():
                    for copy in fetch(quarter(s + 1), t):
                        copy.start()

            for moment in BOTH:
                @pl.when(top & is_inner & (turn == moment))
                def _():
                    early_piece(s, moment).start()

            engine(e + turn)

        loop(2, tile)

        @pl.when(jnp.logical_not(top))
        def _():
            fetch_act(q).wait()
            settle(s - SLOTS)
            pl.semaphore_wait(pcredit)

        once = 1 + lax.div(s, ITEMS)

        def down_part(_):
            value = dot_at(big[:, 2 * Q : 3 * Q], dy_v[...]).astype(bf16).reshape(2, 2, 2, R, D)
            for h in BOTH:
                for core in BOTH:
                    own[slot, 4:6, core, :, D * h : D * h + D] = value[core, :, h]

        loop(once, down_part)
        swap(s, 0).start()

        @pl.when((s >= 3) & (s < ITEMS - 1))
        def _():
            fetch_act(quarter(s + 1)).start()

        engine(e + 2)

        def gate_part(_):
            own[slot, 0:4, :, :, 0:EDGE] = dot_at(a_v[l], big[:, 0:EDGE]).astype(bf16).reshape(4, 2, R, EDGE)

        loop(once, gate_part)
        swap(s, 1).start()
        engine(e + 3)
        own[slot, 0:4, :, :, EDGE:WIDE] = dot_at(a_v[l], big[:, EDGE:WIDE]).astype(bf16).reshape(4, 2, R, EVEN)
        swap(s, 2).start()
        engine(e + 4)

        @pl.when(top)
        def _():
            def tile(t):
                r = rows(t, TM)
                da_v[r] += dot_bt(big[r, 0 : 2 * Q], wgu_v[at])

            loop(tiles, tile)

        engine(e + 5)

        @pl.when((s >= SLOTS - 1) & (s < ITEMS - 1))
        def _():
            pl.semaphore_signal(pcredit, device_id=partner)

    loop(ITEMS, step)

    def tail(k):
        @pl.when(is_end & (k == HEAD))
        def _():
            for copy in hand():
                copy.start()

        engine(6 * ITEMS + k)

    loop(HEAD + 3 * LAG, tail)

    def exchange(k, of):
        return pltpu.make_async_remote_copy(
            part, sums.at[of], sum_send.at[k], sum_recv.at[of], device_id={"dp": lax.rem(me + k, EIGHT)}
        )

    part[...] = sum(ss_v[:, LANES * n : LANES * n + LANES] for n in range(D // LANES))
    for k in OTHERS:
        exchange(k, me).start()
    sums[me] = part[...]
    loop(SLOTS, lambda k: settle(ITEMS - SLOTS + k))
    for k in OTHERS:
        exchange(k, lax.rem(me + k, EIGHT)).wait_recv()
    total = sum(sums[k] for k in range(EIGHT))
    total = jnp.sum(jnp.sum(total, 0, keepdims=True), 1, keepdims=True)
    count = LAYERS * 3 * D * F
    ofac[...] = jnp.broadcast_to(jnp.minimum(1.0, 0.5 * lax.rsqrt(total * (1.0 / count) + 1e-30)), ofac.shape)

    @pl.when(is_end)
    def _():
        for copy in hand():
            copy.wait_send()
        for copy in early_chunks():
            copy.wait_recv()
        for n in range(4):
            for moment in BOTH:
                early_piece(n, moment).wait_recv()

    @pl.when(is_inner)
    def _():
        for copy in hand():
            copy.wait_recv()
        for copy in early_chunks():
            copy.wait_send()
        for n in range(4):
            for moment in BOTH:
                early_piece(n, moment).wait_send()

    for k in OTHERS:
        exchange(k, me).wait_send()


def reduce_gradients(x, dy, w, m, v):
    tokens = x.shape[0]
    hbm, vmem, dma = pl.BlockSpec(memory_space=pl.ANY), pl.BlockSpec(memory_space=pltpu.VMEM), pltpu.SemaphoreType.DMA
    regular = pltpu.SemaphoreType.REGULAR
    return pl.pallas_call(
        step_kernel,
        name="step_kernel",
        out_shape=(
            *[jax.ShapeDtypeStruct((2, LAYERS, R, F), bf16)] * 2,
            jax.ShapeDtypeStruct((2, LAYERS, DROWS, D), bf16),
            jax.ShapeDtypeStruct((EIGHT, LANES), f32),
            *[jax.ShapeDtypeStruct((4, tokens, Q), f32)] * 2,
            jax.ShapeDtypeStruct((4, tokens, Q), bf16),
            *(jax.ShapeDtypeStruct(t, f32) for t in (*CHUNK, *CHUNK, *CHUNK[0:2])),
        ),
        in_specs=[hbm] * 11,
        out_specs=(hbm, hbm, hbm, vmem, *[hbm] * 11),
        scratch_shapes=[
            pltpu.VMEM((tokens, D), bf16),
            pltpu.VMEM((2, tokens, D), bf16),
            pltpu.VMEM((tokens, D), bf16),
            pltpu.VMEM((tokens, F), bf16),
            pltpu.VMEM((2, tokens, D), f32),
            pltpu.VMEM((2, D, 2 * Q), bf16),
            pltpu.VMEM((2, Q, D), bf16),
            pltpu.VMEM((F, D), bf16),
            pltpu.VMEM((SLOTS, 6, 2, R, WIDE), bf16),
            pltpu.VMEM((SLOTS, 6, R, WIDE), bf16),
            pltpu.VMEM((2, PACK, R, D), bf16),
            pltpu.VMEM((EIGHT, D), f32),
            pltpu.VMEM((EIGHT, EIGHT, LANES), f32),
            pltpu.VMEM((EIGHT, LANES), f32),
            dma((4,)),
            dma((2, 4)),
            dma((3, 2)),
            dma((SLOTS, 3)),
            dma((SLOTS, 3)),
            dma((2, SLOTS, EIGHT)),
            dma((2, PACK)),
            dma((SLOTS, 10)),
            *[dma((PACK,))] * 6,
            regular((2,)),
            regular((2,)),
            regular,
        ],
        compiler_params=pltpu.CompilerParams(collective_id=0, has_side_effects=True, vmem_limit_bytes=67043328),
    )(x, dy, *w, *m, *v)


def gather_kernel(
    ofac, emg, emu, emd, evg, evu, evd, ehm, ehv, eg, eu, ed, wg, wu, wd, mg, mu, md, vg, vu, vd, og, ou, od, fg, fu, fd, sg, su, sd,
    gg, gu, gd, bg, bu, bd, xmg, xmu, xmd, xmh, xvg, xvu, xvd, xvh, xgg, xgu, xgd, xgh, xwg, xwu, xwd, xwh, fac,
    fac_sem, x_sem, g_recv, g_send, in_sem, z_send, z_recv, p_send, p_recv, own_sem,
):
    me, z, c, partner = place()
    is_end = at_end(z)
    inner = ahead(me, lax.div(z, 3))
    known = 2, 3, 3
    ends, gs, outs = (eg, eu, ed), (gg, gu, gd), (og, ou, od)
    given = (xmg, xmu, xmd, xmh), (xvg, xvu, xvd, xvh), (xgg, xgu, xgd, xgh), (xwg, xwu, xwd, xwh)

    def layer_half(k):
        return 1 - half(k), odd(k)

    def cut(ref, mat, part, lead, first):
        if mat < 2:
            return ref.at[(*lead, pl.ds(pl.multiple_of(first * R, PACK), R), rows(part, WIDE))]
        return ref.at[(*lead, pl.ds(pl.multiple_of(first * DROWS + part * DHALF, 32), DHALF), slice(None))]

    def state(mat, l):
        n = R if mat < 2 else DROWS
        w = (wg, wu, wd)[mat].at[l, pl.ds(pl.multiple_of(me * n, PACK), n)]
        sources = ((mg, mu, md)[mat].at[l], (vg, vu, vd)[mat].at[l], w)
        return [
            pltpu.make_async_copy(src, there[mat].at[l], in_sem.at[mat, l, n])
            for n, (src, there) in enumerate(zip(sources, ((fg, fu, fd), (sg, su, sd), (bg, bu, bd)), strict=True))
        ]

    def own_g(k, mat):
        l, part = layer_half(k)
        return pltpu.make_async_copy(cut(ends[mat], mat, part, (0, l), 0), cut(gs[mat], mat, part, (l,), 0), own_sem.at[k, mat])

    def hand_g(k, mat):
        l, part = layer_half(k)
        return pltpu.make_async_remote_copy(
            cut(ends[mat], mat, part, (1, l), 0), cut(gs[mat], mat, part, (l,), 0), g_send.at[k, mat], g_recv.at[k, mat],
            device_id=inner,
        )

    def outer(x):
        mat, part = (x, 1) if x < 3 else (0, 0)
        sources = (
            (emg, emu, emd, ehm)[x],
            (evg, evu, evd, ehv)[x],
            cut(ends[mat], mat, part, (1, 0), 0),
            cut((wg, wu, wd)[mat], mat, part, (0,), inner["dp"]),
        )
        return [pltpu.make_async_copy(src, there[x], x_sem.at[x, n]) for n, (src, there) in enumerate(zip(sources, given, strict=True))]

    def chunk(k, mat, block):
        l, part = layer_half(k)
        return cut(outs[mat], mat, part, (l,), block)

    def along(way, hop, k, mat, block):
        ref = chunk(k, mat, block)
        return pltpu.make_async_remote_copy(
            ref, ref, z_send.at[way, hop, k, mat], z_recv.at[way, hop, k, mat], device_id=ahead(me, way)
        )

    def across(k, mat, block):
        ref = chunk(k, mat, block)
        of = half(block)
        return pltpu.make_async_remote_copy(ref, ref, p_send.at[of, k, mat], p_recv.at[of, k, mat], device_id=partner)

    barrier = pltpu.get_barrier_semaphore()
    pl.semaphore_signal(barrier, device_id=partner)

    for way in BOTH:
        @pl.when(z != 3 * flip(way))
        def _():
            pl.semaphore_signal(barrier, device_id=ahead(me, way))

    factor = pltpu.make_async_copy(ofac, fac, fac_sem)
    factor.start()

    def load(l):
        for mat in KINDS:
            for copy in state(mat, l):
                copy.start()

    def take(k):
        @pl.when(is_end | (k == 0))
        def _():
            for mat in KINDS:
                own_g(k, mat).start()

    take(0)
    load(1)
    load(0)
    loop(3, lambda k: take(k + 1))
    pl.semaphore_wait(barrier, 2 + lax.convert_element_type(jnp.logical_not(is_end), jnp.int32))

    @pl.when(is_end)
    def _():
        for x in range(4):
            for copy in outer(x):
                copy.start()

        def hand(k):
            for mat in KINDS:
                hand_g(k + 1, mat).start()

        loop(3, hand)

    factor.wait()

    def stepped(g, w, m, v):
        g = g.astype(f32) * fac[0:1, 0:1]
        w = w.astype(f32)
        m = 0.9 * m + 0.1 * g
        v = 0.95 * v + 0.05 * g * g
        return m, v, (w - 0.02 * (m * lax.rsqrt(v + 1e-8) + 0.1 * w)).astype(bf16)

    def crosses(way, k, mat):
        edge, near = 3 * flip(way), 2 - way
        return (z != edge) & ((z != near) | (k < known[mat]))

    upper = half(z)

    def relay(turn, m, mat):
        way = upper * turn + flip(upper) * flip(turn)
        hop, k = split(m)
        hop = hop + 1
        of = z + hop * (2 * way - 1)
        block = 2 * of + c

        @pl.when((m >= 0) & (m < 12) & (of >= 0) & (of < 4) & ((m >= 4) | (m < known[mat]) | jnp.logical_not(is_end)))
        def _():
            along(way, hop - 1, k, mat, block).wait_recv()

            @pl.when(z != 3 * flip(way))
            def _():
                along(way, hop, k, mat, block).start()

            across(k, mat, block).start()

    def adamw(k):
        l, part = layer_half(k)
        for mat in KINDS:
            relay(0, k - 2, mat)

            @pl.when(part == 0)
            def _():
                for copy in state(mat, l):
                    copy.wait()

            @pl.when(is_end | (k == 0))
            def _():
                own_g(k, mat).wait()

            @pl.when(jnp.logical_not(is_end) & (k > 0))
            def _():
                hand_g(k, mat).wait_recv()

            def piece(n):
                if mat < 2:
                    r, col = rows(n, PACK), rows(part, WIDE)
                    to = (l, pl.ds(pl.multiple_of(me * R + n * PACK, PACK), PACK), col)
                else:
                    r, col = pl.ds(pl.multiple_of(part * DHALF + n * 32, 32), 32), slice(None)
                    to = (l, pl.ds(pl.multiple_of(me * DROWS + part * DHALF + n * 32, 32), 32), col)
                m, v, w = stepped(
                    gs[mat][l, r, col], (bg, bu, bd)[mat][l, r, col], (fg, fu, fd)[mat][l, r, col], (sg, su, sd)[mat][l, r, col]
                )
                (fg, fu, fd)[mat][l, r, col] = m
                (sg, su, sd)[mat][l, r, col] = v
                outs[mat][to] = w

            loop(5, piece)

            for way in (1, 0):
                @pl.when(crosses(way, k, mat))
                def _():
                    along(way, 0, k, mat, me).start()

            across(k, mat, me).start()

    loop(4, adamw)

    @pl.when(is_end)
    def _():
        for x in range(4):
            for copy in outer(x):
                copy.wait()
            mat, part = (x, 1) if x < 3 else (0, 0)

            def piece(n):
                size = PACK if mat < 2 else 2 * PACK
                r = rows(n, size)
                m, v, g, w = (ref[x][r] for ref in given)
                first = inner["dp"] * (R if mat < 2 else DROWS) + n * size + (0 if mat < 2 else DHALF)
                col = slice(WIDE * part, WIDE * part + WIDE) if mat < 2 else slice(None)
                outs[mat][0, pl.ds(pl.multiple_of(first, PACK), size), col] = stepped(g, w, m, v)[2]

            loop(5, piece)
            across(2 + part, mat, inner["dp"]).start()

    far = 3 - z

    def onward(n):
        for mat in KINDS:
            loop(2, lambda turn: relay(turn, n + 2 - 3 * turn, mat))

    def done(of, k):
        for mat in KINDS:
            across(k, mat, 2 * of + c).wait_send()
            across(k, mat, 2 * of + 1 - c).wait_recv()

            @pl.when((of > z) & (z > 0) | (of == z) & crosses(1, k, mat))
            def _():
                along(1, of - z, k, mat, 2 * of + c).wait_send()

            @pl.when((of < z) & (z < 3) | (of == z) & crosses(0, k, mat))
            def _():
                along(0, z - of, k, mat, 2 * of + c).wait_send()

    def finish(n, early):
        of, k = split(n)

        @pl.when(is_end & (of != far) if early else jnp.logical_not(is_end) | (of == far))
        def _():
            done(of, k)

    most = 9
    loop(most, onward)
    loop(PACK, lambda n: finish(n, True))
    loop(4, lambda n: onward(n + most))
    loop(PACK, lambda n: finish(n, False))

    @pl.when(is_end)
    def _():
        def hand(k):
            for mat in KINDS:
                hand_g(k + 1, mat).wait_send()

        loop(3, hand)


def gather_weights(factor, outer, g, w, m, v):
    hbm, vmem, dma = pl.BlockSpec(memory_space=pl.ANY), pl.BlockSpec(memory_space=pltpu.VMEM), pltpu.SemaphoreType.DMA
    block = [(LAYERS, R, F), (LAYERS, R, F), (LAYERS, DROWS, D)]
    return pl.pallas_call(
        gather_kernel,
        name="gather_kernel",
        out_shape=(
            pltpu.VMEM((LAYERS, D, F), bf16),
            pltpu.VMEM((LAYERS, D, F), bf16),
            pltpu.VMEM((LAYERS, F, D), bf16),
            *(pltpu.VMEM(s, f32) for s in block),
            *(pltpu.VMEM(s, f32) for s in block),
        ),
        in_specs=[hbm] * 21,
        out_specs=(vmem,) * 9,
        scratch_shapes=[
            *(pltpu.VMEM(s, bf16) for s in block),
            *(pltpu.VMEM(s, bf16) for s in block),
            *(pltpu.VMEM(s, t) for t in (f32, f32, bf16, bf16) for s in (*CHUNK, CHUNK[0])),
            pltpu.VMEM((EIGHT, LANES), f32),
            dma,
            dma((4, 4)),
            dma((4, 3)),
            dma((4, 3)),
            dma((3, LAYERS, 3)),
            *[dma((2, 4, 4, 3))] * 2,
            *[dma((4, 4, 3))] * 2,
            dma((4, 3)),
        ],
        compiler_params=pltpu.CompilerParams(collective_id=1, has_side_effects=True, vmem_limit_bytes=24 << 20),
    )(*(pltpu.with_memory_space_constraint(t, pltpu.HBM) for t in (factor, *outer, *g, *w, *m, *v)))


def put_kernel(*refs):
    *arrays, sem = refs
    count = len(arrays) // 2
    copies = [pltpu.make_async_copy(arrays[n].at[l], arrays[count + n].at[l], sem.at[n, l]) for n in range(count) for l in range(LAYERS)]
    for copy in copies:
        copy.start()
    for copy in copies:
        copy.wait()


def put(arrays):
    any_space = pl.BlockSpec(memory_space=pl.ANY)
    arrays = [pltpu.with_memory_space_constraint(a, pltpu.VMEM) for a in arrays]
    return pl.pallas_call(
        put_kernel,
        name="put_kernel",
        out_shape=tuple(pltpu.HBM(a.shape, a.dtype) for a in arrays),
        in_specs=[any_space] * len(arrays),
        out_specs=(any_space,) * len(arrays),
        scratch_shapes=[pltpu.SemaphoreType.DMA((len(arrays), LAYERS))],
        compiler_params=pltpu.CompilerParams(vmem_limit_bytes=1 << 20),
    )(*arrays)


def solution(mesh):
    def body(x, dy, *arrays):
        w, m, v = arrays[0:3], arrays[3:6], arrays[6:9]
        results = reduce_gradients(x[0], dy[0], w, m, v)
        return put(gather_weights(results[3], results[7:], results[0:3], w, m, v))

    rep, part = P("rep", None, None), P("rep", "dp", None)
    whole, block = P(None, None, None), P(None, "dp", None)
    seq = P(("rep", "dp"), None, None)
    return jax.shard_map(
        body,
        mesh=mesh,
        in_specs=(seq, seq, *[whole] * 3, *[block] * 6),
        out_specs=(*[rep] * 3, *[part] * 6),
        check_vma=False,
    )
```
